512 devices in a mesh: group: 4 (over z_hi), seq: 16 (over y, core), mp: 8 (over z_lo, x).
Axes of the slice: x: 4, y: 8, z: 8 (z_hi: 4, z_lo: 2; z = z_hi * 2 + z_lo), core: 2. Of those that a mesh axis runs over, the one named last changes fastest.
Arguments:
- patches: bfloat16 [32768, 640], P(('group', 'seq')), may hold values from -6 to 6
- w_merge1: bfloat16 [4, 640, 2560], P(None, 'seq', 'mp'), may hold values from -0.125 to 0.125
- w_merge2: bfloat16 [2560, 4096], P('mp', 'seq'), may hold values from -0.125 to 0.125
- w_query: bfloat16 [4096, 4096], P('seq', 'mp'), may hold values from -0.09375 to 0.09375
- w_keyval: bfloat16 [4096, 2, 1024], P('seq', None, 'mp'), may hold values from -0.09375 to 0.09375
- attn_grad: bfloat16 [8192, 4096], P(('group', 'seq'), 'mp'), may hold values from -6 to 6
- sample_ids: int32 [4, 2048], P('group'), may hold values from 0 to 7, never falling along the last dimension, each value on 1 to 1152 neighbouring positions
Outputs:
- patch_grad: bfloat16 [32768, 640], P(('group', 'seq', 'mp'))
The draws below stay inside these ranges and needn't reach their ends.
Inputs may be any that keep to these rules, and one draw needn't show every extreme that they name: `sample_ids`: in each sequence never falls; every sample spans 1 to 1152 tokens.
All inputs are finite; a program needn't handle non-finite values.
Results may differ from the reference program's by a relative error of at most 0.035.
Values may be sent and summed in bfloat16 or wider, within the bound.
A program may use at most 64 MiB of HBM per device.

```python
import math
import jax
import jax.numpy as jnp
import numpy as np
from jax import lax

V = 640
H = 2560
D = 4096
HEADS = 32
KV_HEADS = 8
HEAD = 128
TOK_SEQ = 128
SAMPLES = 8
RUN = 2048
TOKENS = 8192
PATCHES = 32768
N_GROUP = 4
N_SEQ = 16
N_MP = 8


def block_scale(key, dims, split, least, high):
    factor_of = 1.0
    for position, blocks in split:
        heights = jax.random.uniform(jax.random.fold_in(jax.random.fold_in(key, 6), position), (blocks,), jnp.float32, least / len(split), high / len(split))
        factor_of = factor_of * jnp.repeat(jnp.exp(heights), dims[position] // blocks).reshape((-1,) + (1,) * (len(dims) - 1 - position))
    return factor_of


def length_profile(number_of, total, reach, lean):
    weights = [(1 << 20) // math.isqrt(standing ** lean) + 1 for standing in range(2, number_of + 1)]
    spare, given = total - reach - (number_of - 1), [1] * (number_of - 1)
    while spare > 0:
        candidates = [i for i in range(number_of - 1) if given[i] < reach]
        mass, remaining = sum([weights[i] for i in candidates]), spare
        for i in candidates:
            more = min(reach - given[i], max(1, remaining * weights[i] // mass), spare)
            given[i] = given[i] + more
            spare = spare - more
    return np.array([reach] + given)


def uneven_parts(stream_key, count, total, most, skew):
    if count == 2:
        one = jax.random.randint(stream_key, (), max(1, total - most), min(most, total - 1) + 1)
        return jnp.stack([one, total - one])
    sizes = jnp.asarray(length_profile(count, total, most, skew), jnp.int32)
    pairs = (count - 1) // 2
    donor, receiver = sizes[1:1 + 2 * pairs:2], sizes[2:2 + 2 * pairs:2]
    margin = jnp.minimum(donor - 1, most - receiver)
    moved = jax.random.randint(jax.random.fold_in(stream_key, 1), (pairs,), 0, 1 << 20) % (margin + 1)
    sizes = sizes.at[1:1 + 2 * pairs:2].set(donor - moved).at[2:2 + 2 * pairs:2].set(receiver + moved)
    return sizes[jax.random.permutation(jax.random.fold_in(stream_key, 2), count)]


def bell_draw(key, extent, deviation, limit, cuts=(), kind=jnp.bfloat16):
    gain = block_scale(key, extent, cuts, -0.22, 0.18) if cuts else 1.0
    result = jax.random.normal(key, extent, jnp.float32) * deviation * gain
    return jnp.minimum(jnp.maximum(result, -limit), limit).astype(kind)


def setup_inputs(seed: int = 0) -> dict:
    streams_of = jax.random.split(jax.random.key(seed), 8)
    patches = bell_draw(streams_of[0], (PATCHES, V), 1.0, 6.0, ((0, 64),))
    w_merge1 = bell_draw(streams_of[1], (4, V, H), (4 * V) ** -0.5, 0.125, ((1, 16), (2, 8)))
    w_merge2 = bell_draw(streams_of[2], (H, D), H ** -0.5, 0.125, ((0, 8), (1, 16)))
    w_query = bell_draw(streams_of[3], (D, HEADS * HEAD), D ** -0.5, 0.09375, ((0, 16), (1, 8)))
    w_keyval = bell_draw(streams_of[4], (D, 2, KV_HEADS * HEAD), D ** -0.5, 0.09375, ((0, 16), (2, 8)))
    attn_grad = bell_draw(streams_of[5], (TOKENS, HEADS * HEAD), 1.0, 6.0, ((0, 64), (1, 8)))
    sample_ids = jax.vmap(lambda own: jnp.searchsorted(jnp.cumsum(uneven_parts(own, SAMPLES, RUN, TOK_SEQ * N_SEQ // 2 + TOK_SEQ, 1)), jnp.arange(RUN), side="right"))(jax.random.split(streams_of[6], N_GROUP)).reshape((N_GROUP, RUN)).astype(jnp.int32)
    return {"patches": patches, "w_merge1": w_merge1, "w_merge2": w_merge2, "w_query": w_query, "w_keyval": w_keyval, "attn_grad": attn_grad, "sample_ids": sample_ids}


EPSILON = 1e-06
NEGATIVE = 1e+30

def gelu_grad(inputs):
    normal_cdf = 0.5 * (1.0 + lax.erf(inputs * 0.7071067811865476))
    normal_pdf = jnp.exp(-0.5 * inputs * inputs) * 0.3989422804014327
    return normal_cdf + inputs * normal_pdf

def block_sum(x_blocks, w_blocks):

    def advance(running, operands):
        product = jnp.dot(operands[0], operands[1], preferred_element_type=jnp.float32)
        rounded = lax.optimization_barrier(product.astype(jnp.bfloat16))
        return (running + rounded.astype(jnp.float32), None)
    initial = jnp.zeros((x_blocks.shape[1], w_blocks.shape[2]), jnp.float32)
    running, _ = lax.scan(advance, initial, (x_blocks, w_blocks))
    return running

def split_rows(inputs, blocks):
    return jnp.transpose(inputs.reshape(inputs.shape[0], blocks, inputs.shape[1] // blocks), (1, 0, 2))

def reference(patches, w_merge1, w_merge2, w_query, w_keyval, attn_grad, sample_ids):
    tokens = patches.shape[0] // 4
    run_len = tokens // N_GROUP
    kv_width = KV_HEADS * HEAD
    q_width = HEADS * HEAD
    per_kv = HEADS // KV_HEADS
    score_scale = HEAD ** (-0.5)
    values = patches.astype(jnp.float32)
    row_mean = lax.optimization_barrier(jnp.mean(values, -1, keepdims=True))
    ln_scale = lax.rsqrt(lax.optimization_barrier(jnp.mean(values * values, -1, keepdims=True)) - row_mean * row_mean + EPSILON)
    normed = (values - row_mean) * ln_scale
    merge_in = normed.astype(jnp.bfloat16).reshape(tokens, 4 * V)
    hidden_pre = jnp.dot(merge_in, w_merge1.reshape(4 * V, H), preferred_element_type=jnp.float32)
    hidden = jax.nn.gelu(hidden_pre, approximate=False).astype(jnp.bfloat16)
    merged = block_sum(split_rows(hidden, N_MP), w_merge2.reshape(N_MP, H // N_MP, D)).astype(jnp.bfloat16)
    merged_f = merged.astype(jnp.float32)
    rms_scale = lax.rsqrt(lax.optimization_barrier(jnp.mean(merged_f * merged_f, -1, keepdims=True)) + EPSILON)
    normed_tok = merged_f * rms_scale
    normed_bf = normed_tok.astype(jnp.bfloat16)
    queries = jnp.dot(normed_bf, w_query, preferred_element_type=jnp.float32).astype(jnp.bfloat16)
    keyval = jnp.dot(normed_bf, w_keyval.reshape(D, 2 * kv_width), preferred_element_type=jnp.float32).astype(jnp.bfloat16)

    def to_items(array, tail):
        shaped = array.reshape((N_GROUP, run_len, KV_HEADS) + tail)
        return jnp.moveaxis(shaped, 2, 1).reshape((N_GROUP * KV_HEADS, run_len) + tail)

    def from_items(array, tail, width):
        shaped = array.reshape((N_GROUP, KV_HEADS, run_len) + tail)
        return jnp.moveaxis(shaped, 1, 2).reshape(tokens, width)
    item_queries = to_items(queries, (per_kv, HEAD))
    item_keys = to_items(keyval[:, :kv_width], (HEAD,))
    item_values = to_items(keyval[:, kv_width:], (HEAD,))
    item_grads = to_items(attn_grad, (per_kv, HEAD))
    item_ids = jnp.repeat(sample_ids, KV_HEADS, axis=0)
    positions = jnp.arange(run_len, dtype=jnp.int32)

    def head_grads(operands):
        query_f = operands[0].astype(jnp.float32)
        key_f = operands[1].astype(jnp.float32)
        value_f = operands[2].astype(jnp.float32)
        grad_f = operands[3].astype(jnp.float32)
        ids = operands[4]
        allowed = (positions[:, None] >= positions[None, :]) & (ids[:, None] == ids[None, :])
        scores = jnp.einsum('tgd,ud->gtu', query_f, key_f) * score_scale
        scores = jnp.where(allowed, scores, -NEGATIVE)
        row_max = lax.optimization_barrier(jnp.max(scores, -1, keepdims=True))
        shifted = jnp.exp(scores - row_max)
        soft = shifted / lax.optimization_barrier(jnp.sum(shifted, -1, keepdims=True))
        soft_bf = lax.optimization_barrier(soft.astype(jnp.bfloat16)).astype(jnp.float32)
        attended = jnp.einsum('gtu,ud->tgd', soft_bf, value_f)
        row_delta = lax.optimization_barrier(jnp.sum(grad_f * attended, -1))
        dprob = jnp.einsum('tgd,ud->gtu', grad_f, value_f)
        dscore = soft * (dprob - jnp.transpose(row_delta)[:, :, None])
        dscore = lax.optimization_barrier(dscore.astype(jnp.bfloat16)).astype(jnp.float32)
        dquery = (jnp.einsum('gtu,ud->tgd', dscore, key_f) * score_scale).astype(jnp.bfloat16)
        dkey = (jnp.einsum('gtu,tgd->ud', dscore, query_f) * score_scale).astype(jnp.bfloat16)
        dvalue = jnp.einsum('gtu,tgd->ud', soft_bf, grad_f).astype(jnp.bfloat16)
        return (dquery, dkey, dvalue)
    dquery, dkey, dvalue = lax.map(head_grads, (item_queries, item_keys, item_values, item_grads, item_ids))
    dquery = from_items(dquery, (per_kv, HEAD), q_width)
    dkey = from_items(dkey, (HEAD,), kv_width)
    dvalue = from_items(dvalue, (HEAD,), kv_width)
    group_width = q_width // N_MP
    kv_block = kv_width // N_MP
    dq_blocks = dquery.reshape(tokens, N_MP, group_width)
    dkv = jnp.stack([dkey, dvalue], 1).reshape(tokens, 2, N_MP, kv_block)
    dkv_blocks = jnp.transpose(dkv, (0, 2, 1, 3)).reshape(tokens, N_MP, 2 * kv_block)
    grad_blocks = jnp.transpose(jnp.concatenate([dq_blocks, dkv_blocks], 2), (1, 0, 2))
    wq_blocks = w_query.reshape(D, N_MP, group_width)
    wkv_blocks = jnp.transpose(w_keyval.reshape(D, 2, N_MP, kv_block), (0, 2, 1, 3)).reshape(D, N_MP, 2 * kv_block)
    wcat_blocks = jnp.transpose(jnp.concatenate([wq_blocks, wkv_blocks], 2), (1, 2, 0))
    dnormed = block_sum(grad_blocks, wcat_blocks)
    dmerged = (rms_scale * (dnormed - normed_tok * lax.optimization_barrier(jnp.mean(dnormed * normed_tok, -1, keepdims=True)))).astype(jnp.bfloat16)
    dhidden = jnp.dot(dmerged, jnp.transpose(w_merge2), preferred_element_type=jnp.float32)
    dhidden_pre = (dhidden * gelu_grad(hidden_pre)).astype(jnp.bfloat16)
    w1_blocks = jnp.transpose(w_merge1.reshape(4 * V, N_MP, H // N_MP), (1, 2, 0))
    dmerge_in = block_sum(split_rows(dhidden_pre, N_MP), w1_blocks).reshape(tokens * 4, V)
    first_mean = lax.optimization_barrier(jnp.mean(dmerge_in, -1, keepdims=True))
    second_mean = lax.optimization_barrier(jnp.mean(dmerge_in * normed, -1, keepdims=True))
    patch_grad = ln_scale * (dmerge_in - first_mean - normed * second_mean)
    return patch_grad.astype(jnp.bfloat16)
```

```python
import math

import jax
import jax.numpy as jnp
from jax import lax
from jax.sharding import PartitionSpec as P

HEAD = 128


EPSILON = 1e-06
NEGATIVE = 1e30


def shifted_2(value, axis, steps):
    count = lax.axis_size(axis)
    initial, last = (max(0, -steps), min(count, count - steps))
    return lax.ppermute(value, axis, [(source, source + steps) for source in range(initial, last)])


def copy_for_each(shard, axis):
    copies = jnp.broadcast_to(shard, (lax.axis_size(axis), *shard.shape))
    return lax.all_to_all(copies, axis, split_axis=0, concat_axis=0, tiled=True)


def laid_out(blocks, dim):
    blocks = jnp.moveaxis(blocks, 0, dim)
    lengths = blocks.shape
    return blocks.reshape(*lengths[:dim], lengths[dim] * lengths[dim + 1], *lengths[dim + 2 :])


def gather_directly(shard, axis, dim):
    blocks = copy_for_each(shard, axis)
    return laid_out(blocks, dim)


def split_up(shard, dim, peers):
    before, after = (shard.shape[:dim], shard.shape[dim + 1 :])
    return jnp.moveaxis(shard.reshape(*before, peers, -1, *after), dim, 0)


def sent_and_summed(shard, axis, dim):
    blocks = split_up(shard, dim, lax.axis_size(axis))
    arrived = lax.all_to_all(blocks, axis, split_axis=0, concat_axis=0, tiled=True)
    return arrived.astype(jnp.float32).sum(axis=0)


def side_by_side(arrays, axis, dim, along):
    widths = [math.prod(a.shape[along:]) for a in arrays]
    both = jnp.concatenate(
        [a.reshape(*a.shape[:along], w) for a, w in zip(arrays, widths)], axis=along
    )
    whole = lax.all_gather(both, axis, axis=dim, tiled=True)
    blocks = jnp.split(whole, [sum(widths[:k]) for k in range(1, len(widths))], axis=along)
    return tuple(
        (b.reshape(*whole.shape[:along], *a.shape[along:]) for a, b in zip(arrays, blocks))
    )


def gelu_grad(inputs):
    normal_cdf = 0.5 * (1.0 + lax.erf(inputs * 0.7071067811865476))
    normal_pdf = jnp.exp(-0.5 * inputs * inputs) * 0.3989422804014327
    return normal_cdf + inputs * normal_pdf


def fetch_earlier(own_keyval, offset):
    return shifted_2(own_keyval, "seq", offset)


def return_terms(terms, offset):
    return (
        shifted_2(terms[0].astype(jnp.bfloat16), "seq", -offset).astype(jnp.float32),
        shifted_2(terms[1].astype(jnp.bfloat16), "seq", -offset).astype(jnp.float32),
    )


def local(patches, w_merge1, w_merge2, w_query, w_keyval, attn_grad, sample_ids):
    patch_rows, feat_width = patches.shape
    tok_rows = patch_rows // 4
    score_scale = HEAD ** (-0.5)
    values = patches.astype(jnp.float32)
    row_mean = jnp.mean(values, -1, keepdims=True)
    ln_scale = lax.rsqrt(
        jnp.mean(values * values, -1, keepdims=True) - row_mean * row_mean + EPSILON
    )
    normed = (values - row_mean) * ln_scale
    merge_in = normed.astype(jnp.bfloat16).reshape(tok_rows, 4 * feat_width)
    first_tile = gather_directly(w_merge1, "seq", 1)
    first_flat = first_tile.reshape(4 * feat_width, first_tile.shape[2])
    hidden_pre = jnp.dot(merge_in, first_flat, preferred_element_type=jnp.float32)
    hidden = jax.nn.gelu(hidden_pre, approximate=False).astype(jnp.bfloat16)
    second_tile = lax.all_gather(w_merge2, "seq", axis=1, tiled=True)
    model_width = second_tile.shape[1]
    partial_value = jnp.dot(hidden, second_tile, preferred_element_type=jnp.float32)
    share = sent_and_summed(partial_value.astype(jnp.bfloat16), "mp", 0).astype(jnp.bfloat16)
    merged = gather_directly(share, "mp", 0)
    merged_f = merged.astype(jnp.float32)
    rms_scale = lax.rsqrt(jnp.mean(merged_f * merged_f, -1, keepdims=True) + EPSILON)
    normed_tok = merged_f * rms_scale
    query_tile, keyval_tile = side_by_side((w_query, w_keyval), "seq", 0, 1)
    kv_part = keyval_tile.shape[2]
    keyval_flat = keyval_tile.reshape(model_width, 2 * kv_part)
    normed_bf = normed_tok.astype(jnp.bfloat16)
    queries = jnp.dot(normed_bf, query_tile, preferred_element_type=jnp.float32).astype(
        jnp.bfloat16
    )
    own_keyval = jnp.dot(normed_bf, keyval_flat, preferred_element_type=jnp.float32).astype(
        jnp.bfloat16
    )
    query_part = queries.shape[1]
    kv_local = kv_part // HEAD
    per_kv = query_part // HEAD // kv_local
    run_ids = sample_ids[0]
    run_len = run_ids.shape[0]
    own_start = lax.axis_index("seq") * tok_rows
    reach = min(lax.axis_size("seq") - 1, (run_len // 2 + 2 * tok_rows - 2) // tok_rows)
    pieces = [own_keyval]
    for offset in range(1, reach + 1):
        pieces.insert(0, fetch_earlier(own_keyval, offset))
    window_kv = jnp.concatenate(pieces, 0)
    window_rows = window_kv.shape[0]
    key_pos = own_start - reach * tok_rows + jnp.arange(window_rows, dtype=jnp.int32)
    padded_ids = jnp.concatenate([jnp.full((reach * tok_rows,), -1, jnp.int32), run_ids], 0)
    key_ids = lax.dynamic_slice_in_dim(padded_ids, own_start, window_rows, 0)
    total_rows = window_kv.shape[0]
    key_heads = window_kv[:, :kv_part].reshape(total_rows, kv_local, HEAD)
    value_heads = window_kv[:, kv_part:].reshape(total_rows, kv_local, HEAD)
    query_pos = own_start + jnp.arange(tok_rows, dtype=jnp.int32)
    own_ids = lax.dynamic_slice_in_dim(run_ids, own_start, tok_rows, 0)
    allowed = (query_pos[:, None] >= key_pos[None, :]) & (own_ids[:, None] == key_ids[None, :])
    query_heads = queries.reshape(tok_rows, kv_local, per_kv, HEAD)
    scores = (
        jnp.einsum("tkgd,ukd->kgtu", query_heads, key_heads, preferred_element_type=jnp.float32)
        * score_scale
    )
    scores = jnp.where(allowed, scores, -NEGATIVE)
    row_max = jnp.max(scores, -1, keepdims=True)
    shifted = jnp.exp(scores - row_max)
    soft = shifted / jnp.sum(shifted, -1, keepdims=True)
    soft_bf = soft.astype(jnp.bfloat16)
    attended = jnp.einsum(
        "kgtu,ukd->tkgd", soft_bf, value_heads, preferred_element_type=jnp.float32
    )
    grad_heads = attn_grad.reshape(tok_rows, kv_local, per_kv, HEAD)
    row_delta = jnp.sum(grad_heads.astype(jnp.float32) * attended, -1)
    dprob = jnp.einsum(
        "tkgd,ukd->kgtu", grad_heads, value_heads, preferred_element_type=jnp.float32
    )
    dscore = (soft * (dprob - jnp.transpose(row_delta, (1, 2, 0))[..., None])).astype(jnp.bfloat16)
    dquery = (
        jnp.einsum("kgtu,ukd->tkgd", dscore, key_heads, preferred_element_type=jnp.float32)
        * score_scale
    )
    dquery = dquery.astype(jnp.bfloat16).reshape(tok_rows, query_part)
    dkey_terms = (
        jnp.einsum("kgtu,tkgd->ukd", dscore, query_heads, preferred_element_type=jnp.float32)
        * score_scale
    )
    dvalue_terms = jnp.einsum(
        "kgtu,tkgd->ukd", soft_bf, grad_heads, preferred_element_type=jnp.float32
    )
    dkey = dkey_terms[reach * tok_rows :]
    dvalue = dvalue_terms[reach * tok_rows :]
    for offset in range(1, reach + 1):
        begin_row = (reach - offset) * tok_rows
        key_back, value_back = return_terms(
            (
                dkey_terms[begin_row : begin_row + tok_rows],
                dvalue_terms[begin_row : begin_row + tok_rows],
            ),
            offset,
        )
        dkey = dkey + key_back
        dvalue = dvalue + value_back
    grads_kv = jnp.concatenate(
        [
            dkey.astype(jnp.bfloat16).reshape(tok_rows, kv_part),
            dvalue.astype(jnp.bfloat16).reshape(tok_rows, kv_part),
        ],
        1,
    )
    dnormed_part = jnp.einsum("tc,dc->td", dquery, query_tile, preferred_element_type=jnp.float32)
    dnormed_part = dnormed_part + jnp.einsum(
        "tc,dc->td", grads_kv, keyval_flat, preferred_element_type=jnp.float32
    )
    dnormed = sent_and_summed(dnormed_part.astype(jnp.bfloat16), "mp", 0)
    own_rows = dnormed.shape[0]
    row_start = lax.axis_index("mp") * own_rows
    own_tok = lax.dynamic_slice_in_dim(normed_tok, row_start, own_rows, 0)
    own_rms = lax.dynamic_slice_in_dim(rms_scale, row_start, own_rows, 0)
    inner_mean = jnp.mean(dnormed * own_tok, -1, keepdims=True)
    dmerged_share = (own_rms * (dnormed - own_tok * inner_mean)).astype(jnp.bfloat16)
    dmerged = gather_directly(dmerged_share, "mp", 0)
    dhidden = jnp.einsum("td,hd->th", dmerged, second_tile, preferred_element_type=jnp.float32)
    dhidden_pre = (dhidden * gelu_grad(hidden_pre)).astype(jnp.bfloat16)
    dmerge_part = jnp.einsum(
        "th,fh->tf", dhidden_pre, first_flat, preferred_element_type=jnp.float32
    )
    dmerge_in = sent_and_summed(
        dmerge_part.reshape(patch_rows, feat_width).astype(jnp.bfloat16), "mp", 0
    )
    share_rows = dmerge_in.shape[0]
    begin = lax.axis_index("mp") * share_rows
    own_normed = lax.dynamic_slice_in_dim(normed, begin, share_rows, 0)
    own_scale = lax.dynamic_slice_in_dim(ln_scale, begin, share_rows, 0)
    first_mean = jnp.mean(dmerge_in, -1, keepdims=True)
    second_mean = jnp.mean(dmerge_in * own_normed, -1, keepdims=True)
    patch_grad = own_scale * (dmerge_in - first_mean - own_normed * second_mean)
    return patch_grad.astype(jnp.bfloat16)


def solution(mesh):
    in_specs = (
        P(("group", "seq"), None),
        P(None, "seq", "mp"),
        P("mp", "seq"),
        P("seq", "mp"),
        P("seq", None, "mp"),
        P(("group", "seq"), "mp"),
        P("group", None),
    )
    out_specs = P(("group", "seq", "mp"), None)
    return jax.shard_map(local, mesh=mesh, in_specs=in_specs, out_specs=out_specs, check_vma=False)
```

```python
import functools

import jax
import jax.numpy as jnp
from jax import lax
from jax.experimental import pallas as pl
from jax.experimental.pallas import tpu as pltpu
from jax.sharding import PartitionSpec as P

HEAD = 128
EPSILON = 1e-06
NEGATIVE = 1e30
BF = jnp.bfloat16
F32 = jnp.float32
N_BLOCKS = 10


def gelu_grad(inputs):
    normal_cdf = 0.5 * (1.0 + lax.erf(inputs * 0.7071067811865476))
    normal_pdf = jnp.exp(-0.5 * inputs * inputs) * 0.3989422804014327
    return normal_cdf + inputs * normal_pdf


def dot(a, b):
    return jnp.dot(a, b, preferred_element_type=F32)


def dot_nt(a, b):
    return lax.dot_general(a, b, (((1,), (1,)), ((), ())), preferred_element_type=F32)


def dot_tn(a, b):
    return lax.dot_general(a, b, (((0,), (0,)), ((), ())), preferred_element_type=F32)


def rows(start, count):
    return pl.ds(pl.multiple_of(start, count), count)


def kernel(
    n_seq,
    n_mp,
    patches,
    w1,
    w2,
    wq,
    wkv,
    attn_grad,
    sample_ids,
    out,
    w1g,
    w1n,
    w2g,
    wqg,
    wkvg,
    normed,
    scale,
    hidden_pre,
    hidden,
    part,
    recv,
    merged,
    tok_bf,
    query,
    keys,
    values,
    bias,
    dkeys,
    dvalues,
    ret_send,
    ret_recv,
    chain_send,
    chain_recv,
    blk_send,
    blk_recv,
    dquery,
    grads_kv,
    dn_acc,
    part2,
    recv2,
    dmerged,
    part3,
    recv3,
    out_f32,
    w_send,
    w_recv,
    w_sib,
    rs_send,
    rs_recv,
    kv_send,
    kv_recv,
    ret_ssem,
    ret_rsem,
):
    i = lax.axis_index("seq")
    m = lax.axis_index("mp")
    core = i % 2
    n_chip = n_seq // 2
    sib = i + 1 - 2 * core
    up = (i + 2) % n_seq
    down = (i + n_seq - 2) % n_seq
    far = (i + 9 * core + (n_seq - 9) * (1 - core)) % n_seq
    tok = attn_grad.shape[0]
    share = tok // n_mp
    feat = patches.shape[1]
    fs = feat // n_seq
    dblk = wq.shape[0]

    def seq_copy(src, dst, ssem, rsem, target):
        return pltpu.make_async_remote_copy(
            src_ref=src,
            dst_ref=dst,
            send_sem=ssem,
            recv_sem=rsem,
            device_id={"seq": target},
            device_id_type=pl.DeviceIdType.MESH,
        )

    barrier = pltpu.get_barrier_semaphore()
    for target in (up, down, sib, far):
        pl.semaphore_signal(
            barrier, inc=1, device_id={"seq": target}, device_id_type=pl.DeviceIdType.MESH
        )
    for o in range(1, n_mp):
        pl.semaphore_signal(
            barrier,
            inc=1,
            device_id={"mp": (m + o) % n_mp},
            device_id_type=pl.DeviceIdType.MESH,
        )
    pl.semaphore_wait(barrier, 4 + n_mp - 1)

    sends = []

    own_w = (w1, w2, wq, wkv)
    all_w = (w1g, w2g, wqg, wkvg)
    lead = tuple(None if a.shape[0] == n_seq else o.shape[0] for o, a in zip(own_w, all_w))

    def slot(p, s):
        if lead[p] is None:
            return all_w[p].at[s]
        return all_w[p].at[rows(s * lead[p], lead[p])]

    source = [(i + n_seq - 2 * d) % n_seq for d in (1, 2, 3)]
    source += [(i + 2 * d) % n_seq for d in (1, 2, 3)]
    source += [(i + n_seq // 2) % n_seq]
    sib_source = [(s + 1 - 2 * core) for s in source] + [sib]
    far_up = 1 - core
    turn = (i + 2 * far_up + (n_seq - 2) * (1 - far_up)) % n_seq
    turn_source = (i + (n_seq - 6) * far_up + 6 * (1 - far_up)) % n_seq

    def ring(p, k, s, target):
        return seq_copy(slot(p, s), slot(p, s), w_send.at[p, k], w_recv.at[p, k], target)

    def to_sib(p, k, s):
        return seq_copy(slot(p, s), slot(p, s), w_send.at[p, 7 + k], w_sib.at[p, k], sib)

    def arrived(p, k):
        ring(p, k, source[k], sib).wait_recv()

    def start(copy):
        copy.start()
        sends.append(copy)

    def hop(p, h):
        if h == 1:
            src = own_w[p]
            start(seq_copy(src, slot(p, i), w_send.at[p, 0], w_recv.at[p, 0], up))
            start(seq_copy(src, slot(p, i), w_send.at[p, 3], w_recv.at[p, 3], down))
            start(seq_copy(src, slot(p, i), w_send.at[p, 14], w_sib.at[p, 7], sib))
        elif h <= 3:
            for first, target in ((0, up), (3, down)):
                k = first + h - 2
                arrived(p, k)
                start(ring(p, k + 1, source[k], target))
                start(to_sib(p, k, source[k]))
        elif h == 4:
            for k in (2, 5):
                arrived(p, k)
            start(ring(p, 6, turn_source, turn))
            for k in (2, 5):
                start(to_sib(p, k, source[k]))
        else:
            arrived(p, 6)
            start(to_sib(p, 6, source[6]))

    def gathered(p):
        for k in range(8):
            s = sib_source[k]
            seq_copy(slot(p, s), slot(p, s), w_send.at[p, 7 + k], w_sib.at[p, k], sib).wait_recv()

    def own_slot(p):
        if lead[p] is None:
            all_w[p][i] = own_w[p][...]
        else:
            all_w[p][rows(i * lead[p], lead[p]), :] = own_w[p][...]

    def scatter(step, src, dst):
        for o in range(1, n_mp):
            peer = (m + o) % n_mp
            copy = pltpu.make_async_remote_copy(
                src_ref=src.at[rows(peer * share, share)],
                dst_ref=dst.at[n_mp - o],
                send_sem=rs_send.at[step, o],
                recv_sem=rs_recv.at[step, n_mp - o],
                device_id={"mp": peer},
                device_id_type=pl.DeviceIdType.MESH,
            )
            start(copy)

    def scattered(step, src, dst):
        for o in range(1, n_mp):
            pltpu.make_async_remote_copy(
                src_ref=src.at[rows(m * share, share)],
                dst_ref=dst.at[o],
                send_sem=rs_send.at[step, o],
                recv_sem=rs_recv.at[step, o],
                device_id={"mp": (m + o) % n_mp},
                device_id_type=pl.DeviceIdType.MESH,
            ).wait_recv()

    def spread(step, buf):
        mine = buf.at[rows(m * share, share)]
        for o in range(1, n_mp):
            copy = pltpu.make_async_remote_copy(
                src_ref=mine,
                dst_ref=mine,
                send_sem=rs_send.at[step, o],
                recv_sem=rs_recv.at[step, n_mp - o],
                device_id={"mp": (m + o) % n_mp},
                device_id_type=pl.DeviceIdType.MESH,
            )
            start(copy)

    def spread_done(step, buf):
        for o in range(1, n_mp):
            theirs = buf.at[rows(((m + o) % n_mp) * share, share)]
            pltpu.make_async_remote_copy(
                src_ref=theirs,
                dst_ref=theirs,
                send_sem=rs_send.at[step, o],
                recv_sem=rs_recv.at[step, o],
                device_id={"mp": (m + o) % n_mp},
                device_id_type=pl.DeviceIdType.MESH,
            ).wait_recv()

    def normed_rows(at):
        return jnp.concatenate([normed[j, at, :] for j in range(feat // 128)], 1)

    hop(0, 1)
    hop(1, 1)
    for p in range(4):
        own_slot(p)

    chunk = patches.shape[0] // 4

    @pl.loop(0, 4)
    def _(c):
        at = rows(c * chunk, chunk)
        x = patches[at, :].astype(F32)
        mean = jnp.mean(x, -1, keepdims=True)
        r = lax.rsqrt(jnp.mean(x * x, -1, keepdims=True) - mean * mean + EPSILON)
        x = (x - mean) * r
        for j in range(feat // 128):
            normed[j, at, :] = x[:, j * 128 : (j + 1) * 128]
        scale[at, :] = jnp.broadcast_to(r, (chunk, 128))

    blk_src = [i, (i + (n_seq - 9) * (1 - core) + (n_seq - 1) * core) % n_seq]
    blk_src += [(i + n_seq - 2 * d) % n_seq for d in (1, 2, 3, 4)]
    blk_src += [(i + n_seq - 2 * d + 1 - 2 * core) % n_seq for d in (1, 2, 3, 4)]
    own_ids = sample_ids[0:1, rows(i * tok, tok)]
    q_ids = jnp.transpose(jnp.broadcast_to(own_ids, (tok, tok)))
    row = lax.broadcasted_iota(jnp.int32, (tok, tok), 0)
    lane = lax.broadcasted_iota(jnp.int32, (tok, tok), 1)
    for b in range(N_BLOCKS):
        s = blk_src[b]
        ids = jnp.broadcast_to(sample_ids[0:1, rows(s * tok, tok)], (tok, tok))
        allowed = (ids == q_ids) & (s * tok + lane <= i * tok + row)
        bias[:, b * tok : (b + 1) * tok] = jnp.where(allowed, 0.0, -NEGATIVE)

    hop(0, 2)
    hop(1, 2)
    hop(0, 3)
    hop(1, 3)
    hop(0, 4)
    hop(1, 4)
    hop(0, 5)
    gathered(0)

    for t in range(n_seq // 2):
        a = w1g[2 * t].astype(F32)
        b = w1g[2 * t + 1].astype(F32)
        for p in range(4):
            piece = jnp.concatenate([a[p * fs : (p + 1) * fs], b[p * fs : (p + 1) * fs]], 0)
            w1n[p * feat + 2 * fs * t : p * feat + 2 * fs * (t + 1), :] = piece.astype(BF)

    acc = jnp.zeros((tok, w1.shape[1]), F32)
    for p in range(4):
        x = normed_rows(pl.ds(p, tok, stride=4)).astype(BF)
        acc = acc + dot(x, w1n[p * feat : (p + 1) * feat, :])
    hidden_pre[...] = acc
    hidden[...] = (acc * 0.5 * (1.0 + lax.erf(acc * 0.7071067811865476))).astype(BF)

    hop(1, 5)
    hop(2, 1)
    hop(3, 1)
    gathered(1)
    for s in range(n_seq):
        part[:, s * dblk : (s + 1) * dblk] = dot(hidden[...], w2g[s]).astype(BF)
    scatter(0, part, recv)
    hop(2, 2)
    hop(3, 2)
    scattered(0, part, recv)

    width = part.shape[1]
    n_cols = width // 512 if width % 512 == 0 else 1
    cols = width // n_cols

    @pl.loop(0, n_cols)
    def _(c):
        at = rows(c * cols, cols)
        total = part[rows(m * share, share), at].astype(F32)
        for o in range(1, n_mp):
            total = total + recv[o, :, at].astype(F32)
        merged[rows(m * share, share), at] = total.astype(BF)

    spread(1, merged)
    hop(2, 3)
    hop(3, 3)
    spread_done(1, merged)

    @pl.loop(0, tok // 16)
    def _(c):
        at = rows(c * 16, 16)
        x = merged[at, :].astype(F32)
        r = lax.rsqrt(jnp.mean(x * x, -1, keepdims=True) + EPSILON)
        tok_bf[at, :] = (x * r).astype(BF)

    hop(2, 4)
    hop(3, 4)
    hop(2, 5)
    hop(3, 5)
    gathered(3)
    kv = dot(tok_bf[...], wkvg[...])
    keys[0:tok, :] = kv[:, :HEAD].astype(BF)
    values[0:tok, :] = kv[:, HEAD:].astype(BF)

    near = core * ((i + 9) % n_seq) + (1 - core) * sib

    def kv_copy(which, src_block, dst_block, sem, target):
        buf = (keys, values)[which]
        return seq_copy(
            buf.at[src_block * tok : (src_block + 1) * tok],
            buf.at[dst_block * tok : (dst_block + 1) * tok],
            kv_send.at[which, sem],
            kv_recv.at[which, dst_block],
            target,
        )

    for which in (0, 1):
        start(kv_copy(which, 0, 2, 0, up))
        start(kv_copy(which, 0, 1, 1, near))
    gathered(2)
    qw = wq.shape[1]
    per_kv = qw // HEAD
    for h in range(per_kv):
        at = slice(h * HEAD, (h + 1) * HEAD)
        query[h * tok : (h + 1) * tok, :] = dot(tok_bf[...], wqg[:, at]).astype(BF)
    for d in (1, 2, 3, 4):
        for which in (0, 1):
            kv_copy(which, 1 + d, 1 + d, 0, up).wait_recv()
            if d < 4:
                start(kv_copy(which, 1 + d, 2 + d, 1 + d, up))
            start(kv_copy(which, 1 + d, 5 + d, 4 + d, sib))
    for which in (0, 1):
        for b in (1, 6, 7, 8, 9):
            kv_copy(which, b, b, 0, sib).wait_recv()

    score_scale = HEAD ** (-0.5)
    dkeys[...] = jnp.zeros_like(dkeys)
    dvalues[...] = jnp.zeros_like(dvalues)

    for h in range(per_kv):
        at = slice(h * HEAD, (h + 1) * HEAD)
        q = query[h * tok : (h + 1) * tok, :]
        g = attn_grad[:, at]
        s = dot_nt(q, keys[...]) * score_scale + bias[...]
        e = jnp.exp(s - jnp.max(s, -1, keepdims=True))
        soft = e / jnp.sum(e, -1, keepdims=True)
        soft_bf = soft.astype(BF)
        attended = dot(soft_bf, values[...])
        delta = jnp.sum(g.astype(F32) * attended, -1, keepdims=True)
        dprob = dot_nt(g, values[...])
        ds = (soft * (dprob - delta)).astype(BF)
        dquery[:, at] = (dot(ds, keys[...]) * score_scale).astype(BF)
        dkeys[...] += dot_tn(ds, q) * score_scale
        dvalues[...] += dot_tn(soft_bf, g)

    grads = (dkeys, dvalues)
    back = core * sib + (1 - core) * far

    def ret_copy(which, target):
        return seq_copy(
            ret_send.at[which], ret_recv.at[which], ret_ssem.at[which, 0], ret_rsem.at[which, 0], target
        )

    def blk_copy(which, target):
        return seq_copy(
            blk_send.at[which], blk_recv.at[which], ret_ssem.at[which, 1], ret_rsem.at[which, 1], target
        )

    def chain_copy(which, d, target):
        return seq_copy(
            chain_send.at[which, d - 1],
            chain_recv.at[which, d - 1],
            ret_ssem.at[which, 1 + d],
            ret_rsem.at[which, 1 + d],
            target,
        )

    for which in (0, 1):
        ret_send[which] = grads[which][6 * tok :, :].astype(BF)
        start(ret_copy(which, sib))
    for which in (0, 1):
        blk_send[which] = grads[which][tok : 2 * tok, :].astype(BF)
        start(blk_copy(which, back))

    def chain_step(which, d):
        if d == 4:
            ret_copy(which, sib).wait_recv()
        total = grads[which][(1 + d) * tok : (2 + d) * tok, :]
        total = total + ret_recv[which, (d - 1) * tok : d * tok, :].astype(F32)
        if d < 4:
            chain_copy(which, d + 1, down).wait_recv()
            total = total + chain_recv[which, d].astype(F32)
        chain_send[which, d - 1] = total.astype(BF)
        start(chain_copy(which, d, down))

    for which in (0, 1):
        chain_step(which, 4)
    for quarter in range(4):
        for s in range(quarter * n_seq // 4, (quarter + 1) * n_seq // 4):
            at = slice(s * dblk, (s + 1) * dblk)
            dn_acc[:, at] = dot_nt(dquery[...], wqg[at, :])
        if quarter < 3:
            for which in (0, 1):
                chain_step(which, 3 - quarter)
    for which in (0, 1):
        blk_copy(which, sib).wait_recv()
        chain_copy(which, 1, down).wait_recv()
        total = grads[which][0:tok, :] + blk_recv[which].astype(F32) + chain_recv[which, 0].astype(F32)
        grads_kv[:, which * HEAD : (which + 1) * HEAD] = total.astype(BF)

    for s in range(n_seq):
        at = slice(s * dblk, (s + 1) * dblk)
        part2[:, at] = (dn_acc[:, at] + dot_nt(grads_kv[...], wkvg[at, :])).astype(BF)
    scatter(2, part2, recv2)
    scattered(2, part2, recv2)
    mine = rows(m * share, share)
    x = merged[mine, :].astype(F32)
    r = lax.rsqrt(jnp.mean(x * x, -1, keepdims=True) + EPSILON)
    x = x * r
    dn = part2[mine, :].astype(F32)
    for o in range(1, n_mp):
        dn = dn + recv2[o].astype(F32)
    dmerged[mine, :] = (r * (dn - x * jnp.mean(dn * x, -1, keepdims=True))).astype(BF)
    spread(3, dmerged)
    spread_done(3, dmerged)

    acc = jnp.zeros((tok, w1.shape[1]), F32)
    for s in range(n_seq):
        acc = acc + dot_nt(dmerged[:, s * dblk : (s + 1) * dblk], w2g[s])
    dhidden = (acc * gelu_grad(hidden_pre[...])).astype(BF)
    for p in range(4):
        part3[:, p * feat : (p + 1) * feat] = dot_nt(dhidden, w1n[p * feat : (p + 1) * feat, :]).astype(BF)
    scatter(4, part3, recv3)
    scattered(4, part3, recv3)
    for p in range(4):
        at = slice(p * feat, (p + 1) * feat)
        dx = part3[mine, at].astype(F32)
        for o in range(1, n_mp):
            dx = dx + recv3[o, :, at].astype(F32)
        own = pl.ds(m * (4 * share) + p, share, stride=4)
        nx = normed_rows(own)
        first = jnp.mean(dx, -1, keepdims=True)
        second = jnp.mean(dx * nx, -1, keepdims=True)
        dx = scale[own, :][:, 0:1] * (dx - first - nx * second)
        for j in range(feat // 128):
            out_f32[j, pl.ds(p, share, stride=4), :] = dx[:, j * 128 : (j + 1) * 128]
    for j in range(feat // 128):
        out[:, j * 128 : (j + 1) * 128] = out_f32[j].astype(BF)

    for copy in sends:
        copy.wait_send()


def local(patches, w_merge1, w_merge2, w_query, w_keyval, attn_grad, sample_ids):
    n_seq, n_mp = lax.axis_size("seq"), lax.axis_size("mp")
    w1 = w_merge1.reshape(-1, w_merge1.shape[2])
    wkv = w_keyval.reshape(w_keyval.shape[0], -1)
    tok = attn_grad.shape[0]
    share = tok // n_mp
    feat = patches.shape[1]
    hid = w1.shape[1]
    width = n_seq * w_query.shape[0]
    qw = w_query.shape[1]
    span = N_BLOCKS * tok
    scratch = [
        pltpu.VMEM((n_seq, *w1.shape), BF),
        pltpu.VMEM((4 * feat, hid), BF),
        pltpu.VMEM((n_seq, *w_merge2.shape), BF),
        pltpu.VMEM((width, qw), BF),
        pltpu.VMEM((width, 2 * HEAD), BF),
        pltpu.VMEM((feat // 128, 4 * tok, 128), F32),
        pltpu.VMEM((4 * tok, 128), F32),
        pltpu.VMEM((tok, hid), F32),
        pltpu.VMEM((tok, hid), BF),
        pltpu.VMEM((tok, width), BF),
        pltpu.VMEM((n_mp, share, width), BF),
        pltpu.VMEM((tok, width), BF),
        pltpu.VMEM((tok, width), BF),
        pltpu.VMEM((qw // HEAD * tok, HEAD), BF),
        pltpu.VMEM((span, HEAD), BF),
        pltpu.VMEM((span, HEAD), BF),
        pltpu.VMEM((tok, span), F32),
        pltpu.VMEM((span, HEAD), F32),
        pltpu.VMEM((span, HEAD), F32),
        pltpu.VMEM((2, 4 * tok, HEAD), BF),
        pltpu.VMEM((2, 4 * tok, HEAD), BF),
        pltpu.VMEM((2, 4, tok, HEAD), BF),
        pltpu.VMEM((2, 4, tok, HEAD), BF),
        pltpu.VMEM((2, tok, HEAD), BF),
        pltpu.VMEM((2, tok, HEAD), BF),
        pltpu.VMEM((tok, qw), BF),
        pltpu.VMEM((tok, 2 * HEAD), BF),
        pltpu.VMEM((tok, width), F32),
        pltpu.VMEM((tok, width), BF),
        pltpu.VMEM((n_mp, share, width), BF),
        pltpu.VMEM((tok, width), BF),
        pltpu.VMEM((tok, 4 * feat), BF),
        pltpu.VMEM((n_mp, share, 4 * feat), BF),
        pltpu.VMEM((feat // 128, 4 * share, 128), F32),
        pltpu.SemaphoreType.DMA((4, 15)),
        pltpu.SemaphoreType.DMA((4, 7)),
        pltpu.SemaphoreType.DMA((4, 8)),
        pltpu.SemaphoreType.DMA((5, n_mp)),
        pltpu.SemaphoreType.DMA((5, n_mp)),
        pltpu.SemaphoreType.DMA((2, 9)),
        pltpu.SemaphoreType.DMA((2, N_BLOCKS)),
        pltpu.SemaphoreType.DMA((2, 6)),
        pltpu.SemaphoreType.DMA((2, 6)),
    ]
    vmem = pl.BlockSpec(memory_space=pltpu.VMEM)
    return pl.pallas_call(
        functools.partial(kernel, n_seq, n_mp),
        out_shape=jax.ShapeDtypeStruct((4 * share, feat), BF),
        in_specs=[vmem] * 7,
        out_specs=vmem,
        scratch_shapes=scratch,
        compiler_params=pltpu.CompilerParams(
            collective_id=0, has_side_effects=True, vmem_limit_bytes=56 * 1024 * 1024
        ),
        name="merger",
    )(patches, w1, w_merge2, w_query, wkv, attn_grad, sample_ids)


def solution(mesh):
    in_specs = (
        P(("group", "seq"), None),
        P(None, "seq", "mp"),
        P("mp", "seq"),
        P("seq", "mp"),
        P("seq", None, "mp"),
        P(("group", "seq"), "mp"),
        P("group", None),
    )
    out_specs = P(("group", "seq", "mp"), None)
    return jax.shard_map(local, mesh=mesh, in_specs=in_specs, out_specs=out_specs, check_vma=False)
```

```python
import functools

import jax
import jax.numpy as jnp
from jax import lax
from jax.experimental import pallas as pl
from jax.experimental.pallas import tpu as pltpu
from jax.sharding import PartitionSpec as P

HEAD = 128
EPSILON = 1e-06
NEGATIVE = 1e30
BF = jnp.bfloat16
F32 = jnp.float32
N_BLOCKS = 10


def gelu_grad(inputs):
    normal_cdf = 0.5 * (1.0 + lax.erf(inputs * 0.7071067811865476))
    normal_pdf = jnp.exp(-0.5 * inputs * inputs) * 0.3989422804014327
    return normal_cdf + inputs * normal_pdf


def dot(a, b):
    return jnp.dot(a, b, preferred_element_type=F32)


def dot_nt(a, b):
    return lax.dot_general(a, b, (((1,), (1,)), ((), ())), preferred_element_type=F32)


def dot_tn(a, b):
    return lax.dot_general(a, b, (((0,), (0,)), ((), ())), preferred_element_type=F32)


def rows(start, count):
    return pl.ds(pl.multiple_of(start, count), count)


def kernel(
    n_seq,
    n_mp,
    patches_hbm,
    w1_hbm,
    w2_hbm,
    wq_hbm,
    wkv_hbm,
    attn_grad_hbm,
    sample_ids,
    out,
    patches,
    attn_grad,
    wkv_raw,
    wkv_f32,
    w1g,
    w1n,
    w2g,
    wqg,
    wkvg,
    normed,
    scale,
    hidden_pre,
    hidden,
    part,
    recv,
    merged,
    tok_bf,
    query,
    keys,
    values,
    bias,
    dkeys,
    dvalues,
    ret_send,
    ret_recv,
    chain_send,
    chain_recv,
    blk_send,
    blk_recv,
    kv_relay,
    ret_relay,
    dquery,
    grads_kv,
    dn_acc,
    part2,
    recv2,
    dmerged,
    part3,
    recv3,
    out_f32,
    in_sem,
    w_send,
    w_recv,
    w_sib,
    rs_send,
    rs_recv,
    kv_send,
    kv_recv,
    ret_ssem,
    ret_rsem,
):
    i = lax.axis_index("seq")
    m = lax.axis_index("mp")
    core = i % 2
    sib = i + 1 - 2 * core
    up = (i + 2) % n_seq
    down = (i + n_seq - 2) % n_seq
    up2 = (i + 4) % n_seq
    down2 = (i + n_seq - 4) % n_seq
    far = (i + 9 * core + (n_seq - 9) * (1 - core)) % n_seq
    tok, qw = attn_grad.shape
    share = tok // n_mp
    feat = patches.shape[1]
    fs = feat // n_seq
    hid = hidden.shape[1]
    dblk = w2g.shape[2]
    mine = rows(m * share, share)

    def seq_copy(src, dst, ssem, rsem, target):
        return pltpu.make_async_remote_copy(
            src_ref=src,
            dst_ref=dst,
            send_sem=ssem,
            recv_sem=rsem,
            device_id={"seq": target},
            device_id_type=pl.DeviceIdType.MESH,
        )

    barrier = pltpu.get_barrier_semaphore()
    for target in (up, down, up2, down2, sib, far):
        pl.semaphore_signal(
            barrier, inc=1, device_id={"seq": target}, device_id_type=pl.DeviceIdType.MESH
        )
    for o in range(1, n_mp):
        pl.semaphore_signal(
            barrier,
            inc=1,
            device_id={"mp": (m + o) % n_mp},
            device_id_type=pl.DeviceIdType.MESH,
        )

    groups = [(range(0, 3)), (range(3, 5)), (range(5, 7)), (range(7, 8))]
    spans = [slice(2 * g[0] * dblk, (2 * g[-1] + 2) * dblk) for g in groups]

    half2 = w2g.shape[1] // 2
    rq = wqg.shape[0] // n_seq
    W1, W2A, W2B, WKV, WQA, WQB = range(6)

    def slot(p, s):
        if p == W1:
            return w1g.at[s]
        if p in (W2A, W2B):
            return w2g.at[s, pl.ds((p - W2A) * half2, half2)]
        if p == WKV:
            return wkvg.at[rows(s * rq, rq)]
        return wqg.at[pl.ds(pl.multiple_of(s * rq + (p - WQA) * (rq // 2), rq // 2), rq // 2)]

    own_q = wqg.at[rows(core * rq, rq)]
    loads = [
        pltpu.make_async_copy(w1_hbm, w1g.at[core], in_sem.at[0]),
        pltpu.make_async_copy(w2_hbm, w2g.at[core], in_sem.at[1]),
        pltpu.make_async_copy(patches_hbm, patches, in_sem.at[2]),
        pltpu.make_async_copy(wkv_hbm, wkv_raw, in_sem.at[3]),
        pltpu.make_async_copy(wq_hbm, own_q, in_sem.at[4]),
        pltpu.make_async_copy(attn_grad_hbm, attn_grad, in_sem.at[5]),
    ]
    for load in loads:
        load.start()
    loads[0].wait()
    loads[1].wait()
    pl.semaphore_wait(barrier, 6 + n_mp - 1)

    def slots(p, count):
        if p == W1:
            return w1g.at[pl.ds(0, count)]
        if p in (W2A, W2B):
            return w2g.at[pl.ds(0, count), pl.ds((p - W2A) * half2, half2)]
        if p == WKV:
            return wkvg.at[pl.ds(0, count * rq)]
        return wqg.at[pl.ds(0, count * (rq // 2))]

    def ring(p, src_place, dst_place, target):
        seq_copy(
            slot(p, 2 * src_place + core),
            slot(p, 2 * dst_place + core),
            w_send.at[p],
            w_recv.at[p, (dst_place - 1) // 2],
            target,
        ).start()

    def sib_sem(p, place):
        if p == W1:
            return w_sib.at[0]
        if p in (W2A, W2B):
            return w_sib.at[1 + [k for k in range(4) if place in groups[k]][0]]
        return w_sib.at[5 if p == WKV else 6]

    def to_sib(p, place):
        ref = slot(p, 2 * place + core)
        seq_copy(ref, ref, w_send.at[p], sib_sem(p, place), sib).start()

    def arrived(p, step):
        ref = slots(p, 1 if step == 3 else 2)
        seq_copy(ref, ref, w_send.at[p], w_recv.at[p, step], sib).wait_recv()

    turn = core * down + (1 - core) * up

    def hop(p, h):
        if h == 1:
            ring(p, 0, 1, up)
            ring(p, 0, 2, down)
            to_sib(p, 0)
            return
        arrived(p, h - 2)
        if h <= 3:
            ring(p, 2 * h - 3, 2 * h - 1, up)
            ring(p, 2 * h - 2, 2 * h, down)
        elif h == 4:
            ring(p, 5 + core, 7, turn)
        if h <= 4:
            to_sib(p, 2 * h - 3)
            to_sib(p, 2 * h - 2)
        else:
            to_sib(p, 7)

    def gathered(ref, sem):
        seq_copy(ref, ref, w_send.at[0], w_sib.at[sem], sib).wait_recv()

    def mp_copy(step, src, dst, peer):
        return pltpu.make_async_remote_copy(
            src_ref=src,
            dst_ref=dst,
            send_sem=rs_send.at[step],
            recv_sem=rs_recv.at[step],
            device_id={"mp": peer},
            device_id_type=pl.DeviceIdType.MESH,
        )

    mp_sent = []

    def scatter(step, src, dst, at):
        for o in range(1, n_mp):
            peer = (m + o) % n_mp
            theirs = rows(peer * share, share)
            mp_copy(step, src.at[theirs, at], dst.at[n_mp - o, :, at], peer).start()
        mp_sent.append((step, dst.at[pl.ds(1, n_mp - 1), :, at]))

    def scattered(step, dst, at):
        ref = dst.at[pl.ds(1, n_mp - 1), :, at]
        mp_copy(step, ref, ref, (m + 1) % n_mp).wait_recv()

    def total(src, dst, at):
        value = src[mine, at].astype(F32)
        for o in range(1, n_mp):
            value = value + dst[o, :, at].astype(F32)
        return value

    def spread(step, buf, at):
        ref = buf.at[mine, at]
        for o in range(1, n_mp):
            mp_copy(step, ref, ref, (m + o) % n_mp).start()
        mp_sent.append((step, buf.at[pl.ds(0, (n_mp - 1) * share), at]))

    def spread_done(step, buf, at):
        ref = buf.at[pl.ds(0, (n_mp - 1) * share), at]
        mp_copy(step, ref, ref, (m + 1) % n_mp).wait_recv()

    def normed_rows(at):
        return jnp.concatenate([normed[j, at, :] for j in range(feat // 128)], 1)

    hop(W1, 1)
    hop(W2A, 1)

    chunk = patches.shape[0] // 4
    loads[2].wait()

    @pl.loop(0, 4)
    def _(c):
        at = rows(c * chunk, chunk)
        x = patches[at, :].astype(F32)
        mean = jnp.mean(x, -1, keepdims=True)
        r = lax.rsqrt(jnp.mean(x * x, -1, keepdims=True) - mean * mean + EPSILON)
        x = (x - mean) * r
        for j in range(feat // 128):
            normed[j, at, :] = x[:, j * 128 : (j + 1) * 128]
        scale[at, :] = jnp.broadcast_to(r, (chunk, 128))

    loads[3].wait()
    wkv_f32[...] = wkv_raw[...].astype(F32)
    for which in (0, 1):
        shard = wkv_f32[pl.ds(which, rq, stride=2), :].astype(BF)
        wkvg[rows(core * rq, rq), which * HEAD : (which + 1) * HEAD] = shard

    hop(W1, 2)
    hop(W2B, 1)

    blk_src = [i, (i + (n_seq - 9) * (1 - core) + (n_seq - 1) * core) % n_seq]
    blk_src += [(i + n_seq - 2 * d) % n_seq for d in (1, 2, 3, 4)]
    blk_src += [(i + n_seq - 2 * d + 1 - 2 * core) % n_seq for d in (1, 2, 3, 4)]
    own_ids = sample_ids[0:1, rows(i * tok, tok)]
    q_ids = jnp.transpose(jnp.broadcast_to(own_ids, (tok, tok)))
    row = lax.broadcasted_iota(jnp.int32, (tok, tok), 0)
    lane = lax.broadcasted_iota(jnp.int32, (tok, tok), 1)
    for b in range(N_BLOCKS):
        s = blk_src[b]
        ids = jnp.broadcast_to(sample_ids[0:1, rows(s * tok, tok)], (tok, tok))
        allowed = (ids == q_ids) & (s * tok + lane <= i * tok + row)
        bias[:, b * tok : (b + 1) * tok] = jnp.where(allowed, 0.0, -NEGATIVE)

    hop(W1, 3)
    hop(W2A, 2)
    hop(W1, 4)
    hop(W2B, 2)
    hop(W1, 5)
    hop(W2A, 3)
    hop(W2B, 3)
    loads[4].wait()
    hop(WKV, 1)
    gathered(slots(W1, 8), 0)

    for place, step in enumerate((0, -1, 1, -2, 2, -3, 3, 4)):
        chip = (i // 2 + n_seq // 2 + step) % (n_seq // 2)
        a = w1g[2 * place].astype(F32)
        b = w1g[2 * place + 1].astype(F32)
        for p in range(4):
            piece = jnp.concatenate([a[p * fs : (p + 1) * fs], b[p * fs : (p + 1) * fs]], 0)
            at = pl.ds(pl.multiple_of(p * feat + 2 * fs * chip, 2 * fs), 2 * fs)
            w1n[at, :] = piece.astype(BF)

    acc = jnp.zeros((tok, hid), F32)
    for p in range(4):
        x = normed_rows(pl.ds(p, tok, stride=4)).astype(BF)
        acc = acc + dot(x, w1n[p * feat : (p + 1) * feat, :])
    hidden_pre[...] = acc
    hidden[...] = (acc * 0.5 * (1.0 + lax.erf(acc * 0.7071067811865476))).astype(BF)

    def merge_group(g):
        gathered(w2g.at[pl.ds(0, len(groups[g]))], 1 + g)
        for s in range(2 * groups[g][0], 2 * groups[g][-1] + 2):
            part[:, s * dblk : (s + 1) * dblk] = dot(hidden[...], w2g[s]).astype(BF)
        scatter(g, part, recv, spans[g])

    merge_group(0)
    hop(W2A, 4)
    hop(W2B, 4)
    hop(WQA, 1)
    merge_group(1)
    hop(WKV, 2)
    merge_group(2)
    hop(W2A, 5)
    hop(W2B, 5)
    merge_group(3)
    hop(WQA, 2)

    def sum_group(g):
        scattered(g, recv, spans[g])
        for s in range(spans[g].start, spans[g].stop, 2 * dblk):
            at = slice(s, s + 2 * dblk)
            merged[mine, at] = total(part, recv, at).astype(BF)
        spread(4 + g, merged, spans[g])

    sum_group(0)
    hop(WKV, 3)
    sum_group(1)
    hop(WQB, 1)
    sum_group(2)
    hop(WKV, 4)
    sum_group(3)
    hop(WQA, 3)
    hop(WKV, 5)
    hop(WQB, 2)
    hop(WQA, 4)
    for g in range(4):
        spread_done(4 + g, merged, spans[g])

    @pl.loop(0, tok // 16)
    def _(c):
        at = rows(c * 16, 16)
        x = merged[at, :].astype(F32)
        r = lax.rsqrt(jnp.mean(x * x, -1, keepdims=True) + EPSILON)
        tok_bf[at, :] = (x * r).astype(BF)

    hop(WQB, 3)
    gathered(slots(WKV, 8), 5)
    kv = dot(tok_bf[...], wkvg[...])
    keys[0:tok, :] = kv[:, :HEAD].astype(BF)
    values[0:tok, :] = kv[:, HEAD:].astype(BF)

    near = core * ((i + 9) % n_seq) + (1 - core) * sib

    def block(buf, b):
        return buf.at[b * tok : (b + 1) * tok]

    def kv_copy(which, src, dst, arrive, target):
        return seq_copy(src, dst, kv_send.at[which], kv_recv.at[which, arrive], target)

    def kv_step(d):
        for which in (0, 1):
            buf = (keys, values)[which]
            ref = block(buf, 1 + d)
            kv_copy(which, ref, ref, d, sib).wait_recv()
            if d == 1:
                kv_copy(which, ref, block(buf, 4), 3, up2).start()
            kv_copy(which, ref, block(buf, 5 + d), 5, sib).start()

    for which in (0, 1):
        own = block((keys, values)[which], 0)
        kv_copy(which, own, block((keys, values)[which], 2), 1, up).start()
        kv_copy(which, own, kv_relay.at[which], 0, down2).start()
    for which in (0, 1):
        own = block((keys, values)[which], 0)
        kv_copy(which, own, block((keys, values)[which], 3), 2, up2).start()
        kv_copy(which, own, block((keys, values)[which], 1), 5, near).start()
    kv_step(1)
    for which in (0, 1):
        ref = kv_relay.at[which]
        kv_copy(which, ref, ref, 0, sib).wait_recv()
        kv_copy(which, ref, block((keys, values)[which], 5), 4, down2).start()
    hop(WQA, 5)
    hop(WQB, 4)
    kv_step(2)
    kv_step(3)
    kv_step(4)
    hop(WQB, 5)
    gathered(wqg.at[pl.ds(0, 8 * rq)], 6)
    per_kv = qw // HEAD
    for h in range(per_kv):
        at = slice(h * HEAD, (h + 1) * HEAD)
        query[h * tok : (h + 1) * tok, :] = dot(tok_bf[...], wqg[:, at]).astype(BF)
    for which in (0, 1):
        ref = (keys, values)[which].at[0 : 5 * tok]
        kv_copy(which, ref, ref, 5, sib).wait_recv()

    loads[5].wait()
    score_scale = HEAD ** (-0.5)
    dkeys[...] = jnp.zeros_like(dkeys)
    dvalues[...] = jnp.zeros_like(dvalues)

    for h in range(per_kv):
        at = slice(h * HEAD, (h + 1) * HEAD)
        q = query[h * tok : (h + 1) * tok, :]
        g = attn_grad[:, at]
        s = dot_nt(q, keys[...]) * score_scale + bias[...]
        e = jnp.exp(s - jnp.max(s, -1, keepdims=True))
        soft = e / jnp.sum(e, -1, keepdims=True)
        soft_bf = soft.astype(BF)
        attended = dot(soft_bf, values[...])
        delta = jnp.sum(g.astype(F32) * attended, -1, keepdims=True)
        dprob = dot_nt(g, values[...])
        ds = (soft * (dprob - delta)).astype(BF)
        dquery[:, at] = (dot(ds, keys[...]) * score_scale).astype(BF)
        dkeys[...] += dot_tn(ds, q) * score_scale
        dvalues[...] += dot_tn(soft_bf, g)

    grads = (dkeys, dvalues)
    back = core * sib + (1 - core) * far

    def ret_copy(which, src, dst, arrive, target):
        return seq_copy(src, dst, ret_ssem.at[which], ret_rsem.at[which, arrive], target)

    def ret_wait(which, ref, arrive):
        ret_copy(which, ref, ref, arrive, sib).wait_recv()

    for which in (0, 1):
        ret_send[which] = grads[which][6 * tok :, :].astype(BF)
        ret_copy(which, ret_send.at[which], ret_recv.at[which], 0, sib).start()
    for which in (0, 1):
        blk_send[which] = grads[which][tok : 2 * tok, :].astype(BF)
        ret_copy(which, blk_send.at[which], blk_recv.at[which], 1, back).start()

    def chain_step(which, d):
        value = grads[which][(1 + d) * tok : (2 + d) * tok, :]
        value = value + ret_recv[which, (d - 1) * tok : d * tok, :].astype(F32)
        if d == 1:
            ret_wait(which, chain_recv.at[which, 2], 4)
            value = value + chain_recv[which, 2].astype(F32)
        chain_send[which, d - 1] = value.astype(BF)
        src, dst = chain_send.at[which, d - 1], chain_recv.at[which, d - 1]
        if d == 4:
            ret_copy(which, src, ret_relay.at[which], 6, up2).start()
        else:
            ret_copy(which, src, dst, 1 + d, down if d == 1 else down2).start()

    for which in (0, 1):
        ret_wait(which, ret_recv.at[which], 0)
        chain_step(which, 3)
        chain_step(which, 4)
    for which in (0, 1):
        chain_step(which, 2)
    half = n_seq // 2
    for s in range(half):
        at = slice(s * dblk, (s + 1) * dblk)
        dn_acc[:, at] = dot_nt(dquery[...], wqg[at, :])
    for which in (0, 1):
        chain_step(which, 1)
    for which in (0, 1):
        ret_wait(which, ret_relay.at[which], 6)
        ret_copy(which, ret_relay.at[which], chain_recv.at[which, 3], 5, up2).start()
    for s in range(half, n_seq):
        at = slice(s * dblk, (s + 1) * dblk)
        dn_acc[:, at] = dot_nt(dquery[...], wqg[at, :])
    for which in (0, 1):
        ret_wait(which, blk_recv.at[which], 1)
        value = grads[which][0:tok, :] + blk_recv[which].astype(F32)
        for d in (2, 4, 1):
            ret_wait(which, chain_recv.at[which, d - 1], 1 + d)
            value = value + chain_recv[which, d - 1].astype(F32)
        grads_kv[:, which * HEAD : (which + 1) * HEAD] = value.astype(BF)

    for g in range(4):
        for s in range(2 * groups[g][0], 2 * groups[g][-1] + 2):
            at = slice(s * dblk, (s + 1) * dblk)
            part2[:, at] = (dn_acc[:, at] + dot_nt(grads_kv[...], wkvg[at, :])).astype(BF)
        scatter(8 + g, part2, recv2, spans[g])
    for g in range(4):
        scattered(8 + g, recv2, spans[g])
    x = merged[mine, :].astype(F32)
    r = lax.rsqrt(jnp.mean(x * x, -1, keepdims=True) + EPSILON)
    x = x * r
    dn = total(part2, recv2, slice(0, n_seq * dblk))
    dmerged[mine, :] = (r * (dn - x * jnp.mean(dn * x, -1, keepdims=True))).astype(BF)
    for g in range(4):
        spread(12 + g, dmerged, spans[g])
    acc = jnp.zeros((tok, hid), F32)
    for g in range(4):
        spread_done(12 + g, dmerged, spans[g])
        for s in range(2 * groups[g][0], 2 * groups[g][-1] + 2):
            acc = acc + dot_nt(dmerged[:, s * dblk : (s + 1) * dblk], w2g[s])
    dhidden = (acc * gelu_grad(hidden_pre[...])).astype(BF)
    pieces = [slice(p * feat, (p + 1) * feat) for p in range(4)]
    for p in range(4):
        part3[:, pieces[p]] = dot_nt(dhidden, w1n[pieces[p], :]).astype(BF)
        scatter(16 + p, part3, recv3, pieces[p])
    for p in range(4):
        scattered(16 + p, recv3, pieces[p])
        dx = total(part3, recv3, pieces[p])
        own = pl.ds(m * (4 * share) + p, share, stride=4)
        nx = normed_rows(own)
        first = jnp.mean(dx, -1, keepdims=True)
        second = jnp.mean(dx * nx, -1, keepdims=True)
        dx = scale[own, :][:, 0:1] * (dx - first - nx * second)
        for j in range(feat // 128):
            out_f32[j, pl.ds(p, share, stride=4), :] = dx[:, j * 128 : (j + 1) * 128]
    for j in range(feat // 128):
        out[:, j * 128 : (j + 1) * 128] = out_f32[j].astype(BF)

    for p in range(6):
        seq_copy(slots(p, 15), slots(p, 15), w_send.at[p], w_recv.at[p, 0], sib).wait_send()
    for step, ref in mp_sent:
        mp_copy(step, ref, ref, (m + 1) % n_mp).wait_send()
    for which in (0, 1):
        kv_copy(which, keys, keys, 0, sib).wait_send()
        ret_copy(which, keys, keys, 0, sib).wait_send()


def local(patches, w_merge1, w_merge2, w_query, w_keyval, attn_grad, sample_ids):
    n_seq, n_mp = lax.axis_size("seq"), lax.axis_size("mp")
    w1 = w_merge1.reshape(-1, w_merge1.shape[2])
    wkv = w_keyval.reshape(-1, HEAD)
    tok = attn_grad.shape[0]
    share = tok // n_mp
    feat = patches.shape[1]
    hid = w1.shape[1]
    width = n_seq * w_query.shape[0]
    qw = w_query.shape[1]
    span = N_BLOCKS * tok
    scratch = [
        pltpu.VMEM(patches.shape, BF),
        pltpu.VMEM(attn_grad.shape, BF),
        pltpu.VMEM(wkv.shape, BF),
        pltpu.VMEM(wkv.shape, F32),
        pltpu.VMEM((n_seq, *w1.shape), BF),
        pltpu.VMEM((4 * feat, hid), BF),
        pltpu.VMEM((n_seq, *w_merge2.shape), BF),
        pltpu.VMEM((width, qw), BF),
        pltpu.VMEM((width, 2 * HEAD), BF),
        pltpu.VMEM((feat // 128, 4 * tok, 128), F32),
        pltpu.VMEM((4 * tok, 128), F32),
        pltpu.VMEM((tok, hid), F32),
        pltpu.VMEM((tok, hid), BF),
        pltpu.VMEM((tok, width), BF),
        pltpu.VMEM((n_mp, share, width), BF),
        pltpu.VMEM((tok, width), BF),
        pltpu.VMEM((tok, width), BF),
        pltpu.VMEM((qw // HEAD * tok, HEAD), BF),
        pltpu.VMEM((span, HEAD), BF),
        pltpu.VMEM((span, HEAD), BF),
        pltpu.VMEM((tok, span), F32),
        pltpu.VMEM((span, HEAD), F32),
        pltpu.VMEM((span, HEAD), F32),
        pltpu.VMEM((2, 4 * tok, HEAD), BF),
        pltpu.VMEM((2, 4 * tok, HEAD), BF),
        pltpu.VMEM((2, 4, tok, HEAD), BF),
        pltpu.VMEM((2, 4, tok, HEAD), BF),
        pltpu.VMEM((2, tok, HEAD), BF),
        pltpu.VMEM((2, tok, HEAD), BF),
        pltpu.VMEM((2, tok, HEAD), BF),
        pltpu.VMEM((2, tok, HEAD), BF),
        pltpu.VMEM((tok, qw), BF),
        pltpu.VMEM((tok, 2 * HEAD), BF),
        pltpu.VMEM((tok, width), F32),
        pltpu.VMEM((tok, width), BF),
        pltpu.VMEM((n_mp, share, width), BF),
        pltpu.VMEM((tok, width), BF),
        pltpu.VMEM((tok, 4 * feat), BF),
        pltpu.VMEM((n_mp, share, 4 * feat), BF),
        pltpu.VMEM((feat // 128, 4 * share, 128), F32),
        pltpu.SemaphoreType.DMA((6,)),
        pltpu.SemaphoreType.DMA((6,)),
        pltpu.SemaphoreType.DMA((6, 4)),
        pltpu.SemaphoreType.DMA((7,)),
        pltpu.SemaphoreType.DMA((20,)),
        pltpu.SemaphoreType.DMA((20,)),
        pltpu.SemaphoreType.DMA((2,)),
        pltpu.SemaphoreType.DMA((2, 6)),
        pltpu.SemaphoreType.DMA((2,)),
        pltpu.SemaphoreType.DMA((2, 7)),
    ]
    vmem = pl.BlockSpec(memory_space=pltpu.VMEM)
    return pl.pallas_call(
        functools.partial(kernel, n_seq, n_mp),
        out_shape=jax.ShapeDtypeStruct((4 * share, feat), BF),
        in_specs=[pl.BlockSpec(memory_space=pl.ANY)] * 6 + [vmem],
        out_specs=vmem,
        scratch_shapes=scratch,
        compiler_params=pltpu.CompilerParams(
            collective_id=0, has_side_effects=True, vmem_limit_bytes=56 * 1024 * 1024
        ),
        name="merger",
    )(patches, w1, w_merge2, w_query, wkv, attn_grad, sample_ids)


def solution(mesh):
    in_specs = (
        P(("group", "seq"), None),
        P(None, "seq", "mp"),
        P("mp", "seq"),
        P("seq", "mp"),
        P("seq", None, "mp"),
        P(("group", "seq"), "mp"),
        P("group", None),
    )
    out_specs = P(("group", "seq", "mp"), None)
    return jax.shard_map(local, mesh=mesh, in_specs=in_specs, out_specs=out_specs, check_vma=False)
```

```python
import functools

import jax
import jax.numpy as jnp
from jax import lax
from jax.experimental import pallas as pl
from jax.experimental.pallas import tpu as pltpu
from jax.sharding import PartitionSpec as P

HEAD = 128
EPSILON = 1e-06
NEGATIVE = 1e30
BF = jnp.bfloat16
F32 = jnp.float32
N_BLOCKS = 10


def gelu_grad(inputs):
    normal_cdf = 0.5 * (1.0 + lax.erf(inputs * 0.7071067811865476))
    normal_pdf = jnp.exp(-0.5 * inputs * inputs) * 0.3989422804014327
    return normal_cdf + inputs * normal_pdf


def dot(a, b):
    return jnp.dot(a, b, preferred_element_type=F32)


def dot_nt(a, b):
    return lax.dot_general(a, b, (((1,), (1,)), ((), ())), preferred_element_type=F32)


def dot_tn(a, b):
    return lax.dot_general(a, b, (((0,), (0,)), ((), ())), preferred_element_type=F32)


def rows(start, count):
    return pl.ds(pl.multiple_of(start, count), count)


def kernel(
    n_seq,
    n_mp,
    patches_hbm,
    w1_hbm,
    w2_hbm,
    wq_hbm,
    wkv_hbm,
    attn_grad_hbm,
    sample_ids,
    out,
    patches,
    attn_grad,
    wkv_raw,
    wkv_f32,
    w1g,
    w1n,
    w2g,
    wqg,
    wkvg,
    normed,
    scale,
    hidden_pre,
    hidden,
    part,
    recv,
    merged,
    tok_bf,
    query,
    keys,
    values,
    bias,
    dkeys,
    dvalues,
    ret_send,
    ret_recv,
    chain_send,
    chain_recv,
    blk_send,
    blk_recv,
    kv_relay,
    ret_relay,
    dquery,
    grads_kv,
    dn_acc,
    part2,
    recv2,
    sum2,
    dmerged,
    part3,
    recv3,
    out_f32,
    in_sem,
    w_send,
    w_recv,
    w_sib,
    rs_send,
    rs_recv,
    kv_send,
    kv_recv,
    ret_ssem,
    ret_rsem,
):
    i = lax.axis_index("seq")
    m = lax.axis_index("mp")
    core = i % 2
    sib = i + 1 - 2 * core
    up = (i + 2) % n_seq
    down = (i + n_seq - 2) % n_seq
    up2 = (i + 4) % n_seq
    down2 = (i + n_seq - 4) % n_seq
    far = (i + 9 * core + (n_seq - 9) * (1 - core)) % n_seq
    tok, qw = attn_grad.shape
    share = tok // n_mp
    feat = patches.shape[1]
    fs = feat // n_seq
    hid = hidden.shape[1]
    dblk = w2g.shape[2]
    mine = rows(m * share, share)

    def seq_copy(src, dst, ssem, rsem, target):
        return pltpu.make_async_remote_copy(
            src_ref=src,
            dst_ref=dst,
            send_sem=ssem,
            recv_sem=rsem,
            device_id={"seq": target},
            device_id_type=pl.DeviceIdType.MESH,
        )

    barrier = pltpu.get_barrier_semaphore()
    for target in (up, down, up2, down2, sib, far):
        pl.semaphore_signal(
            barrier, inc=1, device_id={"seq": target}, device_id_type=pl.DeviceIdType.MESH
        )
    for o in range(1, n_mp):
        pl.semaphore_signal(
            barrier,
            inc=1,
            device_id={"mp": (m + o) % n_mp},
            device_id_type=pl.DeviceIdType.MESH,
        )

    groups = [(range(0, 3)), (range(3, 5)), (range(5, 7)), (range(7, 8))]
    spans = [slice(2 * g[0] * dblk, (2 * g[-1] + 2) * dblk) for g in groups]

    half2 = w2g.shape[1] // 2
    rq = wqg.shape[0] // n_seq
    W1, W2A, W2B, WKV, WQA, WQB = range(6)

    def slot(p, s):
        if p == W1:
            return w1g.at[s]
        if p in (W2A, W2B):
            return w2g.at[s, pl.ds((p - W2A) * half2, half2)]
        if p == WKV:
            return wkvg.at[rows(s * rq, rq)]
        return wqg.at[pl.ds(pl.multiple_of(s * rq + (p - WQA) * (rq // 2), rq // 2), rq // 2)]

    own_q = wqg.at[rows(core * rq, rq)]
    loads = [
        pltpu.make_async_copy(w1_hbm, w1g.at[core], in_sem.at[0]),
        pltpu.make_async_copy(w2_hbm, w2g.at[core], in_sem.at[1]),
        pltpu.make_async_copy(patches_hbm, patches, in_sem.at[2]),
        pltpu.make_async_copy(wkv_hbm, wkv_raw, in_sem.at[3]),
        pltpu.make_async_copy(wq_hbm, own_q, in_sem.at[4]),
        pltpu.make_async_copy(attn_grad_hbm, attn_grad, in_sem.at[5]),
    ]
    for load in loads:
        load.start()
    loads[0].wait()
    loads[1].wait()
    pl.semaphore_wait(barrier, 6 + n_mp - 1)

    def slots(p, count):
        if p == W1:
            return w1g.at[pl.ds(0, count)]
        if p in (W2A, W2B):
            return w2g.at[pl.ds(0, count), pl.ds((p - W2A) * half2, half2)]
        if p == WKV:
            return wkvg.at[pl.ds(0, count * rq)]
        return wqg.at[pl.ds(0, count * (rq // 2))]

    def ring(p, src_place, dst_place, target):
        seq_copy(
            slot(p, 2 * src_place + core),
            slot(p, 2 * dst_place + core),
            w_send.at[p],
            w_recv.at[p, (dst_place - 1) // 2],
            target,
        ).start()

    def sib_sem(p, place):
        if p == W1:
            return w_sib.at[0]
        if p in (W2A, W2B):
            return w_sib.at[1 + [k for k in range(4) if place in groups[k]][0]]
        return w_sib.at[5 if p == WKV else 6]

    def to_sib(p, place):
        ref = slot(p, 2 * place + core)
        seq_copy(ref, ref, w_send.at[p], sib_sem(p, place), sib).start()

    def arrived(p, step):
        ref = slots(p, 1 if step == 3 else 2)
        seq_copy(ref, ref, w_send.at[p], w_recv.at[p, step], sib).wait_recv()

    turn = core * down + (1 - core) * up

    def hop(p, h):
        if h == 1:
            ring(p, 0, 1, up)
            ring(p, 0, 2, down)
            to_sib(p, 0)
            return
        arrived(p, h - 2)
        if h <= 3:
            ring(p, 2 * h - 3, 2 * h - 1, up)
            ring(p, 2 * h - 2, 2 * h, down)
        elif h == 4:
            ring(p, 5 + core, 7, turn)
        if h <= 4:
            to_sib(p, 2 * h - 3)
            to_sib(p, 2 * h - 2)
        else:
            to_sib(p, 7)

    def gathered(ref, sem):
        seq_copy(ref, ref, w_send.at[0], w_sib.at[sem], sib).wait_recv()

    def mp_copy(step, src, dst, peer):
        return pltpu.make_async_remote_copy(
            src_ref=src,
            dst_ref=dst,
            send_sem=rs_send.at[step],
            recv_sem=rs_recv.at[step],
            device_id={"mp": peer},
            device_id_type=pl.DeviceIdType.MESH,
        )

    mp_sent = []

    def scatter(step, src, dst, at):
        for o in range(1, n_mp):
            peer = (m + o) % n_mp
            theirs = rows(peer * share, share)
            mp_copy(step, src.at[theirs, at], dst.at[n_mp - o, :, at], peer).start()
        mp_sent.append((step, dst.at[pl.ds(1, n_mp - 1), :, at]))

    def scattered(step, dst, at):
        ref = dst.at[pl.ds(1, n_mp - 1), :, at]
        mp_copy(step, ref, ref, (m + 1) % n_mp).wait_recv()

    def total(src, dst, at):
        value = src[mine, at].astype(F32)
        for o in range(1, n_mp):
            value = value + dst[o, :, at].astype(F32)
        return value

    def spread(step, buf, at):
        ref = buf.at[mine, at]
        for o in range(1, n_mp):
            mp_copy(step, ref, ref, (m + o) % n_mp).start()
        mp_sent.append((step, buf.at[pl.ds(0, (n_mp - 1) * share), at]))

    def spread_done(step, buf, at):
        ref = buf.at[pl.ds(0, (n_mp - 1) * share), at]
        mp_copy(step, ref, ref, (m + 1) % n_mp).wait_recv()

    def normed_rows(at):
        return jnp.concatenate([normed[j, at, :] for j in range(feat // 128)], 1)

    hop(W1, 1)
    hop(W2A, 1)

    chunk = patches.shape[0] // 4
    loads[2].wait()

    @pl.loop(0, 4)
    def _(c):
        at = rows(c * chunk, chunk)
        x = patches[at, :].astype(F32)
        mean = jnp.mean(x, -1, keepdims=True)
        r = lax.rsqrt(jnp.mean(x * x, -1, keepdims=True) - mean * mean + EPSILON)
        x = (x - mean) * r
        for j in range(feat // 128):
            normed[j, at, :] = x[:, j * 128 : (j + 1) * 128]
        scale[at, :] = jnp.broadcast_to(r, (chunk, 128))

    loads[3].wait()
    wkv_f32[...] = wkv_raw[...].astype(F32)
    for which in (0, 1):
        shard = wkv_f32[pl.ds(which, rq, stride=2), :].astype(BF)
        wkvg[rows(core * rq, rq), which * HEAD : (which + 1) * HEAD] = shard

    hop(W1, 2)
    hop(W2B, 1)

    blk_src = [i, (i + (n_seq - 9) * (1 - core) + (n_seq - 1) * core) % n_seq]
    blk_src += [(i + n_seq - 2 * d) % n_seq for d in (1, 2, 3, 4)]
    blk_src += [(i + n_seq - 2 * d + 1 - 2 * core) % n_seq for d in (1, 2, 3, 4)]
    own_ids = sample_ids[0:1, rows(i * tok, tok)]
    q_ids = jnp.transpose(jnp.broadcast_to(own_ids, (tok, tok)))
    row = lax.broadcasted_iota(jnp.int32, (tok, tok), 0)
    lane = lax.broadcasted_iota(jnp.int32, (tok, tok), 1)
    for b in range(N_BLOCKS):
        s = blk_src[b]
        ids = jnp.broadcast_to(sample_ids[0:1, rows(s * tok, tok)], (tok, tok))
        allowed = (ids == q_ids) & (s * tok + lane <= i * tok + row)
        bias[:, b * tok : (b + 1) * tok] = jnp.where(allowed, 0.0, -NEGATIVE)

    hop(W1, 3)
    hop(W2A, 2)
    hop(W1, 4)
    hop(W2B, 2)
    hop(W1, 5)
    hop(W2A, 3)
    hop(W2B, 3)
    loads[4].wait()
    hop(WKV, 1)
    gathered(slots(W1, 8), 0)

    for place, step in enumerate((0, -1, 1, -2, 2, -3, 3, 4)):
        chip = (i // 2 + n_seq // 2 + step) % (n_seq // 2)
        a = w1g[2 * place].astype(F32)
        b = w1g[2 * place + 1].astype(F32)
        for p in range(4):
            piece = jnp.concatenate([a[p * fs : (p + 1) * fs], b[p * fs : (p + 1) * fs]], 0)
            at = pl.ds(pl.multiple_of(p * feat + 2 * fs * chip, 2 * fs), 2 * fs)
            w1n[at, :] = piece.astype(BF)

    acc = jnp.zeros((tok, hid), F32)
    for p in range(4):
        x = normed_rows(pl.ds(p, tok, stride=4)).astype(BF)
        acc = acc + dot(x, w1n[p * feat : (p + 1) * feat, :])
    hidden_pre[...] = acc
    hidden[...] = (acc * 0.5 * (1.0 + lax.erf(acc * 0.7071067811865476))).astype(BF)

    def merge_group(g):
        gathered(w2g.at[pl.ds(0, len(groups[g]))], 1 + g)
        for s in range(2 * groups[g][0], 2 * groups[g][-1] + 2):
            part[:, s * dblk : (s + 1) * dblk] = dot(hidden[...], w2g[s]).astype(BF)
        scatter(g, part, recv, spans[g])

    merge_group(0)
    hop(W2A, 4)
    hop(W2B, 4)
    hop(WQA, 1)
    merge_group(1)
    hop(WKV, 2)
    merge_group(2)
    hop(W2A, 5)
    hop(W2B, 5)
    merge_group(3)
    hop(WQA, 2)

    def sum_group(g):
        scattered(g, recv, spans[g])
        for s in range(spans[g].start, spans[g].stop, 2 * dblk):
            at = slice(s, s + 2 * dblk)
            merged[mine, at] = total(part, recv, at).astype(BF)
        spread(4 + g, merged, spans[g])

    sum_group(0)
    hop(WKV, 3)
    sum_group(1)
    hop(WQB, 1)
    sum_group(2)
    hop(WKV, 4)
    sum_group(3)
    hop(WQA, 3)
    hop(WKV, 5)
    hop(WQB, 2)
    hop(WQA, 4)
    for g in range(4):
        spread_done(4 + g, merged, spans[g])

    @pl.loop(0, tok // 16)
    def _(c):
        at = rows(c * 16, 16)
        x = merged[at, :].astype(F32)
        r = lax.rsqrt(jnp.mean(x * x, -1, keepdims=True) + EPSILON)
        tok_bf[at, :] = (x * r).astype(BF)

    hop(WQB, 3)
    gathered(slots(WKV, 8), 5)
    kv = dot(tok_bf[...], wkvg[...])
    keys[0:tok, :] = kv[:, :HEAD].astype(BF)
    values[0:tok, :] = kv[:, HEAD:].astype(BF)

    near = core * ((i + 9) % n_seq) + (1 - core) * sib

    def block(buf, b):
        return buf.at[b * tok : (b + 1) * tok]

    def kv_copy(which, src, dst, arrive, target):
        return seq_copy(src, dst, kv_send.at[which], kv_recv.at[which, arrive], target)

    def kv_step(d):
        for which in (0, 1):
            buf = (keys, values)[which]
            ref = block(buf, 1 + d)
            kv_copy(which, ref, ref, d, sib).wait_recv()
            if d == 1:
                kv_copy(which, ref, block(buf, 4), 3, up2).start()
            kv_copy(which, ref, block(buf, 5 + d), 5, sib).start()

    for which in (0, 1):
        own = block((keys, values)[which], 0)
        kv_copy(which, own, block((keys, values)[which], 2), 1, up).start()
        kv_copy(which, own, kv_relay.at[which], 0, down2).start()
    for which in (0, 1):
        own = block((keys, values)[which], 0)
        kv_copy(which, own, block((keys, values)[which], 3), 2, up2).start()
        kv_copy(which, own, block((keys, values)[which], 1), 5, near).start()
    kv_step(1)
    hop(WQB, 4)
    for which in (0, 1):
        ref = kv_relay.at[which]
        kv_copy(which, ref, ref, 0, sib).wait_recv()
        kv_copy(which, ref, block((keys, values)[which], 5), 4, down2).start()
    hop(WQA, 5)
    kv_step(2)
    kv_step(3)
    kv_step(4)
    hop(WQB, 5)
    gathered(wqg.at[pl.ds(0, 8 * rq)], 6)
    per_kv = qw // HEAD
    for h in range(per_kv):
        at = slice(h * HEAD, (h + 1) * HEAD)
        query[h * tok : (h + 1) * tok, :] = dot(tok_bf[...], wqg[:, at]).astype(BF)
    for which in (0, 1):
        ref = (keys, values)[which].at[0 : 5 * tok]
        kv_copy(which, ref, ref, 5, sib).wait_recv()

    loads[5].wait()
    score_scale = HEAD ** (-0.5)
    dkeys[...] = jnp.zeros_like(dkeys)
    dvalues[...] = jnp.zeros_like(dvalues)

    for h in range(per_kv):
        at = slice(h * HEAD, (h + 1) * HEAD)
        q = query[h * tok : (h + 1) * tok, :]
        g = attn_grad[:, at]
        s = dot_nt(q, keys[...]) * score_scale + bias[...]
        e = jnp.exp(s - jnp.max(s, -1, keepdims=True))
        soft = e / jnp.sum(e, -1, keepdims=True)
        soft_bf = soft.astype(BF)
        attended = dot(soft_bf, values[...])
        delta = jnp.sum(g.astype(F32) * attended, -1, keepdims=True)
        dprob = dot_nt(g, values[...])
        ds = (soft * (dprob - delta)).astype(BF)
        dquery[:, at] = (dot(ds, keys[...]) * score_scale).astype(BF)
        dkeys[...] += dot_tn(ds, q) * score_scale
        dvalues[...] += dot_tn(soft_bf, g)

    grads = (dkeys, dvalues)
    back = core * sib + (1 - core) * far

    def ret_copy(which, src, dst, arrive, target):
        return seq_copy(src, dst, ret_ssem.at[which], ret_rsem.at[which, arrive], target)

    def ret_wait(which, ref, arrive):
        ret_copy(which, ref, ref, arrive, sib).wait_recv()

    for which in (0, 1):
        ret_send[which] = grads[which][6 * tok :, :].astype(BF)
        ret_copy(which, ret_send.at[which], ret_recv.at[which], 0, sib).start()
    for which in (0, 1):
        blk_send[which] = grads[which][tok : 2 * tok, :].astype(BF)
        ret_copy(which, blk_send.at[which], blk_recv.at[which], 1, back).start()

    def chain_step(which, d):
        value = grads[which][(1 + d) * tok : (2 + d) * tok, :]
        value = value + ret_recv[which, (d - 1) * tok : d * tok, :].astype(F32)
        if d == 1:
            ret_wait(which, chain_recv.at[which, 2], 4)
            value = value + chain_recv[which, 2].astype(F32)
        chain_send[which, d - 1] = value.astype(BF)
        src, dst = chain_send.at[which, d - 1], chain_recv.at[which, d - 1]
        if d == 4:
            ret_copy(which, src, ret_relay.at[which], 6, up2).start()
        else:
            ret_copy(which, src, dst, 1 + d, down if d == 1 else down2).start()

    for which in (0, 1):
        ret_wait(which, ret_recv.at[which], 0)
        chain_step(which, 3)
        chain_step(which, 4)
    for which in (0, 1):
        chain_step(which, 2)
    half = n_seq // 2
    for s in range(half):
        at = slice(s * dblk, (s + 1) * dblk)
        dn_acc[:, at] = dot_nt(dquery[...], wqg[at, :])
    for which in (0, 1):
        chain_step(which, 1)
    for which in (0, 1):
        ret_wait(which, ret_relay.at[which], 6)
        ret_copy(which, ret_relay.at[which], chain_recv.at[which, 3], 5, up2).start()
    for s in range(half, n_seq):
        at = slice(s * dblk, (s + 1) * dblk)
        dn_acc[:, at] = dot_nt(dquery[...], wqg[at, :])
    for which in (0, 1):
        ret_wait(which, blk_recv.at[which], 1)
        value = grads[which][0:tok, :] + blk_recv[which].astype(F32)
        for d in (2, 4, 1):
            ret_wait(which, chain_recv.at[which, d - 1], 1 + d)
            value = value + chain_recv[which, d - 1].astype(F32)
        grads_kv[:, which * HEAD : (which + 1) * HEAD] = value.astype(BF)

    n_x = n_mp // 2
    z, x_id = m // n_x, m % n_x
    z_peer = (m + n_x) % n_mp
    col_b = spans[0]
    col_a = slice(spans[1].start, spans[3].stop)

    def x_peer(o):
        return z * n_x + (x_id + o) % n_x

    def block_rows(zz, xx):
        return rows((zz * n_x + xx) * share, share)

    def rs_copy(src, dst, arrive, peer):
        return pltpu.make_async_remote_copy(
            src_ref=src,
            dst_ref=dst,
            send_sem=rs_send.at[8],
            recv_sem=rs_recv.at[8 + arrive],
            device_id={"mp": peer},
            device_id_type=pl.DeviceIdType.MESH,
        )

    def rs_wait(ref, arrive):
        rs_copy(ref, ref, arrive, z_peer).wait_recv()

    for g in (1, 2, 3, 0):
        for s in range(2 * groups[g][0], 2 * groups[g][-1] + 2):
            at = slice(s * dblk, (s + 1) * dblk)
            part2[:, at] = (dn_acc[:, at] + dot_nt(grads_kv[...], wkvg[at, :])).astype(BF)
        if g > 0:
            for xx in range(n_x):
                rs_copy(
                    part2.at[block_rows(1 - z, xx), spans[g]], recv2.at[xx, :, spans[g]], g, z_peer
                ).start()
        else:
            for o in range(1, n_x):
                for zz in range(2):
                    rs_copy(
                        part2.at[block_rows(zz, (x_id + o) % n_x), col_b],
                        recv2.at[2 * (n_x - o) + zz, :, col_b],
                        0,
                        x_peer(o),
                    ).start()
    def sum_a(xx, at):
        return part2[block_rows(z, xx), at].astype(F32) + recv2[xx, :, at].astype(F32)

    for g in (1, 2, 3):
        rs_wait(recv2.at[pl.ds(0, n_x), :, spans[g]], g)
        for o in range(1, n_x):
            sum2[o, :, spans[g]] = sum_a((x_id + o) % n_x, spans[g]).astype(BF)
            rs_copy(sum2.at[o, :, spans[g]], recv2.at[2 * n_x - o, :, spans[g]], 4, x_peer(o)).start()
    rs_wait(recv2.at[pl.ds(2, 2 * n_x - 2), :, col_b], 0)

    def sum_b(zz):
        value = part2[block_rows(zz, x_id), col_b].astype(F32)
        for o in range(1, n_x):
            value = value + recv2[2 * o + zz, :, col_b].astype(F32)
        return value

    sum2[0, :, col_b] = sum_b(1 - z).astype(BF)
    rs_copy(sum2.at[0, :, col_b], recv2.at[0, :, col_b], 5, z_peer).start()
    dn_a, dn_b = sum_a(x_id, col_a), sum_b(z)
    rs_wait(recv2.at[pl.ds(n_x + 1, n_x - 1), :, col_a], 4)
    for o in range(1, n_x):
        dn_a = dn_a + recv2[n_x + o, :, col_a].astype(F32)
    rs_wait(recv2.at[0, :, col_b], 5)
    dn_b = dn_b + recv2[0, :, col_b].astype(F32)
    x = merged[mine, :].astype(F32)
    r = lax.rsqrt(jnp.mean(x * x, -1, keepdims=True) + EPSILON)
    x = x * r
    dn = jnp.concatenate([dn_b, dn_a], 1)
    dmerged[mine, :] = (r * (dn - x * jnp.mean(dn * x, -1, keepdims=True))).astype(BF)

    def ag_copy(block, at, arrive, peer):
        ref = dmerged.at[block, at]
        return pltpu.make_async_remote_copy(
            src_ref=ref,
            dst_ref=ref,
            send_sem=rs_send.at[9],
            recv_sem=rs_recv.at[20 + arrive],
            device_id={"mp": peer},
            device_id_type=pl.DeviceIdType.MESH,
        )

    ag_copy(mine, col_b, 0, z_peer).start()
    for o in range(1, n_x):
        ag_copy(mine, col_a, n_x - o, x_peer(o)).start()
    ag_copy(mine, col_a, 4, z_peer).start()
    for o in range(1, n_x):
        ag_copy(mine, col_b, 5, x_peer(o)).start()
    theirs = rows(z_peer * share, share)
    ag_copy(theirs, col_b, 0, z_peer).wait_recv()
    for o in range(1, n_x):
        ag_copy(theirs, col_b, 5, x_peer(o)).start()
    for o in (1, 3, 2):
        block_of = rows(x_peer(o) * share, share)
        ag_copy(block_of, col_a, o, z_peer).wait_recv()
        ag_copy(block_of, col_a, 4, z_peer).start()
    acc = jnp.zeros((tok, hid), F32)
    ag_copy(pl.ds(0, (2 * n_x - 2) * share), col_b, 5, z_peer).wait_recv()
    for s in range(2 * groups[0][0], 2 * groups[0][-1] + 2):
        acc = acc + dot_nt(dmerged[:, s * dblk : (s + 1) * dblk], w2g[s])
    ag_copy(pl.ds(0, n_x * share), col_a, 4, z_peer).wait_recv()
    for s in range(2 * groups[1][0], n_seq):
        acc = acc + dot_nt(dmerged[:, s * dblk : (s + 1) * dblk], w2g[s])
    dhidden = (acc * gelu_grad(hidden_pre[...])).astype(BF)
    pieces = [slice(p * feat, (p + 1) * feat) for p in range(4)]
    for p in range(4):
        part3[:, pieces[p]] = dot_nt(dhidden, w1n[pieces[p], :]).astype(BF)
        scatter(16 + p, part3, recv3, pieces[p])
    for p in range(4):
        scattered(16 + p, recv3, pieces[p])
        dx = total(part3, recv3, pieces[p])
        own = pl.ds(m * (4 * share) + p, share, stride=4)
        nx = normed_rows(own)
        first = jnp.mean(dx, -1, keepdims=True)
        second = jnp.mean(dx * nx, -1, keepdims=True)
        dx = scale[own, :][:, 0:1] * (dx - first - nx * second)
        for j in range(feat // 128):
            out_f32[j, pl.ds(p, share, stride=4), :] = dx[:, j * 128 : (j + 1) * 128]
    for j in range(feat // 128):
        out[:, j * 128 : (j + 1) * 128] = out_f32[j].astype(BF)

    for p in range(6):
        seq_copy(slots(p, 15), slots(p, 15), w_send.at[p], w_recv.at[p, 0], sib).wait_send()
    for step, ref in mp_sent:
        mp_copy(step, ref, ref, (m + 1) % n_mp).wait_send()
    both = dmerged.at[pl.ds(0, (n_mp - 1) * share)]
    rs_copy(both, both, 0, z_peer).wait_send()
    ag_copy(pl.ds(0, (n_mp - 1) * share), slice(0, n_seq * dblk), 0, z_peer).wait_send()
    for which in (0, 1):
        kv_copy(which, keys, keys, 0, sib).wait_send()
        ret_copy(which, keys, keys, 0, sib).wait_send()


def local(patches, w_merge1, w_merge2, w_query, w_keyval, attn_grad, sample_ids):
    n_seq, n_mp = lax.axis_size("seq"), lax.axis_size("mp")
    w1 = w_merge1.reshape(-1, w_merge1.shape[2])
    wkv = w_keyval.reshape(-1, HEAD)
    tok = attn_grad.shape[0]
    share = tok // n_mp
    feat = patches.shape[1]
    hid = w1.shape[1]
    width = n_seq * w_query.shape[0]
    qw = w_query.shape[1]
    span = N_BLOCKS * tok
    scratch = [
        pltpu.VMEM(patches.shape, BF),
        pltpu.VMEM(attn_grad.shape, BF),
        pltpu.VMEM(wkv.shape, BF),
        pltpu.VMEM(wkv.shape, F32),
        pltpu.VMEM((n_seq, *w1.shape), BF),
        pltpu.VMEM((4 * feat, hid), BF),
        pltpu.VMEM((n_seq, *w_merge2.shape), BF),
        pltpu.VMEM((width, qw), BF),
        pltpu.VMEM((width, 2 * HEAD), BF),
        pltpu.VMEM((feat // 128, 4 * tok, 128), F32),
        pltpu.VMEM((4 * tok, 128), F32),
        pltpu.VMEM((tok, hid), F32),
        pltpu.VMEM((tok, hid), BF),
        pltpu.VMEM((tok, width), BF),
        pltpu.VMEM((n_mp, share, width), BF),
        pltpu.VMEM((tok, width), BF),
        pltpu.VMEM((tok, width), BF),
        pltpu.VMEM((qw // HEAD * tok, HEAD), BF),
        pltpu.VMEM((span, HEAD), BF),
        pltpu.VMEM((span, HEAD), BF),
        pltpu.VMEM((tok, span), F32),
        pltpu.VMEM((span, HEAD), F32),
        pltpu.VMEM((span, HEAD), F32),
        pltpu.VMEM((2, 4 * tok, HEAD), BF),
        pltpu.VMEM((2, 4 * tok, HEAD), BF),
        pltpu.VMEM((2, 4, tok, HEAD), BF),
        pltpu.VMEM((2, 4, tok, HEAD), BF),
        pltpu.VMEM((2, tok, HEAD), BF),
        pltpu.VMEM((2, tok, HEAD), BF),
        pltpu.VMEM((2, tok, HEAD), BF),
        pltpu.VMEM((2, tok, HEAD), BF),
        pltpu.VMEM((tok, qw), BF),
        pltpu.VMEM((tok, 2 * HEAD), BF),
        pltpu.VMEM((tok, width), F32),
        pltpu.VMEM((tok, width), BF),
        pltpu.VMEM((n_mp, share, width), BF),
        pltpu.VMEM((n_mp // 2, share, width), BF),
        pltpu.VMEM((tok, width), BF),
        pltpu.VMEM((tok, 4 * feat), BF),
        pltpu.VMEM((n_mp, share, 4 * feat), BF),
        pltpu.VMEM((feat // 128, 4 * share, 128), F32),
        pltpu.SemaphoreType.DMA((6,)),
        pltpu.SemaphoreType.DMA((6,)),
        pltpu.SemaphoreType.DMA((6, 4)),
        pltpu.SemaphoreType.DMA((7,)),
        pltpu.SemaphoreType.DMA((20,)),
        pltpu.SemaphoreType.DMA((26,)),
        pltpu.SemaphoreType.DMA((2,)),
        pltpu.SemaphoreType.DMA((2, 6)),
        pltpu.SemaphoreType.DMA((2,)),
        pltpu.SemaphoreType.DMA((2, 7)),
    ]
    vmem = pl.BlockSpec(memory_space=pltpu.VMEM)
    return pl.pallas_call(
        functools.partial(kernel, n_seq, n_mp),
        out_shape=jax.ShapeDtypeStruct((4 * share, feat), BF),
        in_specs=[pl.BlockSpec(memory_space=pl.ANY)] * 6 + [vmem],
        out_specs=vmem,
        scratch_shapes=scratch,
        compiler_params=pltpu.CompilerParams(
            collective_id=0, has_side_effects=True, vmem_limit_bytes=56 * 1024 * 1024
        ),
        name="merger",
    )(patches, w1, w_merge2, w_query, wkv, attn_grad, sample_ids)


def solution(mesh):
    in_specs = (
        P(("group", "seq"), None),
        P(None, "seq", "mp"),
        P("mp", "seq"),
        P("seq", "mp"),
        P("seq", None, "mp"),
        P(("group", "seq"), "mp"),
        P("group", None),
    )
    out_specs = P(("group", "seq", "mp"), None)
    return jax.shard_map(local, mesh=mesh, in_specs=in_specs, out_specs=out_specs, check_vma=False)
```

```python
import functools

import jax
import jax.numpy as jnp
from jax import lax
from jax.experimental import pallas as pl
from jax.experimental.pallas import tpu as pltpu
from jax.sharding import PartitionSpec as P

HEAD = 128
EPSILON = 1e-06
NEGATIVE = 1e30
BF = jnp.bfloat16
F32 = jnp.float32
N_BLOCKS = 10


def gelu_grad(inputs):
    normal_cdf = 0.5 * (1.0 + lax.erf(inputs * 0.7071067811865476))
    normal_pdf = jnp.exp(-0.5 * inputs * inputs) * 0.3989422804014327
    return normal_cdf + inputs * normal_pdf


def dot(a, b):
    return jnp.dot(a, b, preferred_element_type=F32)


def dot_nt(a, b):
    return lax.dot_general(a, b, (((1,), (1,)), ((), ())), preferred_element_type=F32)


def dot_tn(a, b):
    return lax.dot_general(a, b, (((0,), (0,)), ((), ())), preferred_element_type=F32)


def rows(start, count):
    return pl.ds(pl.multiple_of(start, count), count)


def kernel(
    n_seq,
    n_mp,
    patches_hbm,
    w1_hbm,
    w2_hbm,
    wq_hbm,
    wkv_hbm,
    attn_grad_hbm,
    sample_ids,
    out,
    patches,
    attn_grad,
    wkv_raw,
    wkv_f32,
    w1_raw,
    w1g,
    w1n,
    w2g,
    wqg,
    wkvg,
    normed,
    scale,
    hidden_pre,
    hidden,
    part,
    recv,
    merged,
    row_scale,
    query,
    keys,
    values,
    bias,
    dkeys,
    dvalues,
    ret_send,
    ret_recv,
    chain_send,
    chain_recv,
    blk_send,
    blk_recv,
    kv_relay,
    ret_relay,
    dquery,
    grads_kv,
    dn_acc,
    part2,
    recv2,
    sum2,
    dmerged,
    part3,
    recv3,
    out_f32,
    in_sem,
    w_send,
    w_recv,
    w_sib,
    rs_send,
    rs_recv,
    kv_send,
    kv_recv,
    ret_ssem,
    ret_rsem,
):
    i = lax.axis_index("seq")
    m = lax.axis_index("mp")
    core = i % 2
    sib = i + 1 - 2 * core
    up = (i + 2) % n_seq
    down = (i + n_seq - 2) % n_seq
    up2 = (i + 4) % n_seq
    down2 = (i + n_seq - 4) % n_seq
    far = (i + 9 * core + (n_seq - 9) * (1 - core)) % n_seq
    tok, qw = attn_grad.shape
    share = tok // n_mp
    feat = patches.shape[1]
    fs = feat // n_seq
    hid = hidden.shape[1]
    dblk = w2g.shape[2]
    mine = rows(m * share, share)

    def seq_copy(src, dst, ssem, rsem, target):
        return pltpu.make_async_remote_copy(
            src_ref=src,
            dst_ref=dst,
            send_sem=ssem,
            recv_sem=rsem,
            device_id={"seq": target},
            device_id_type=pl.DeviceIdType.MESH,
        )

    barrier = pltpu.get_barrier_semaphore()
    for target in (up, down, up2, down2, sib, far):
        pl.semaphore_signal(
            barrier, inc=1, device_id={"seq": target}, device_id_type=pl.DeviceIdType.MESH
        )
    for o in range(1, n_mp):
        pl.semaphore_signal(
            barrier,
            inc=1,
            device_id={"mp": (m + o) % n_mp},
            device_id_type=pl.DeviceIdType.MESH,
        )

    groups = [(range(0, 3)), (range(3, 5)), (range(5, 7)), (range(7, 8))]
    spans = [slice(2 * g[0] * dblk, (2 * g[-1] + 2) * dblk) for g in groups]

    half2 = w2g.shape[1] // 2
    rq = wqg.shape[0] // n_seq
    W1, W2A, W2B, WKV, WQA, WQB = range(6)

    def slot(p, s):
        if p == W1:
            return w1g.at[s]
        if p in (W2A, W2B):
            return w2g.at[s, pl.ds((p - W2A) * half2, half2)]
        if p == WKV:
            return wkvg.at[rows(s * rq, rq)]
        return wqg.at[pl.ds(pl.multiple_of(s * rq + (p - WQA) * (rq // 2), rq // 2), rq // 2)]

    own_q = wqg.at[rows(core * rq, rq)]
    loads = [
        pltpu.make_async_copy(w1_hbm, w1_raw, in_sem.at[0]),
        pltpu.make_async_copy(w2_hbm, w2g.at[core], in_sem.at[1]),
        pltpu.make_async_copy(patches_hbm, patches, in_sem.at[2]),
        pltpu.make_async_copy(wkv_hbm, wkv_raw, in_sem.at[3]),
        pltpu.make_async_copy(wq_hbm, own_q, in_sem.at[4]),
        pltpu.make_async_copy(attn_grad_hbm, attn_grad, in_sem.at[5]),
    ]
    for load in loads:
        load.start()
    loads[0].wait()
    r1 = w1_raw.shape[0]
    full = hid // 128
    for j in range(full):
        w1g[core, j * r1 : (j + 1) * r1, :] = w1_raw[:, j * 128 : (j + 1) * 128]
    tail = w1_raw[:, full * 128 :].astype(F32)
    w1g[core, full * r1 :, :] = jnp.concatenate([tail[: r1 // 2], tail[r1 // 2 :]], 1).astype(BF)
    loads[1].wait()
    pl.semaphore_wait(barrier, 6 + n_mp - 1)

    def slots(p, count):
        if p == W1:
            return w1g.at[pl.ds(0, count)]
        if p in (W2A, W2B):
            return w2g.at[pl.ds(0, count), pl.ds((p - W2A) * half2, half2)]
        if p == WKV:
            return wkvg.at[pl.ds(0, count * rq)]
        return wqg.at[pl.ds(0, count * (rq // 2))]

    def ring(p, src_place, dst_place, target):
        seq_copy(
            slot(p, 2 * src_place + core),
            slot(p, 2 * dst_place + core),
            w_send.at[p],
            w_recv.at[p, (dst_place - 1) // 2],
            target,
        ).start()

    def sib_sem(p, place):
        if p == W1:
            return w_sib.at[0]
        if p in (W2A, W2B):
            return w_sib.at[1 + [k for k in range(4) if place in groups[k]][0]]
        return w_sib.at[5 if p == WKV else 6]

    def to_sib(p, place):
        ref = slot(p, 2 * place + core)
        seq_copy(ref, ref, w_send.at[p], sib_sem(p, place), sib).start()

    def arrived(p, step):
        ref = slots(p, 1 if step == 3 else 2)
        seq_copy(ref, ref, w_send.at[p], w_recv.at[p, step], sib).wait_recv()

    turn = core * down + (1 - core) * up

    def hop(p, h):
        if h == 1:
            ring(p, 0, 1, up)
            ring(p, 0, 2, down)
            to_sib(p, 0)
            return
        arrived(p, h - 2)
        if h <= 3:
            ring(p, 2 * h - 3, 2 * h - 1, up)
            ring(p, 2 * h - 2, 2 * h, down)
        elif h == 4:
            ring(p, 5 + core, 7, turn)
        if h <= 4:
            to_sib(p, 2 * h - 3)
            to_sib(p, 2 * h - 2)
        else:
            to_sib(p, 7)

    def gathered(ref, sem):
        seq_copy(ref, ref, w_send.at[0], w_sib.at[sem], sib).wait_recv()

    def mp_copy(step, src, dst, peer):
        return pltpu.make_async_remote_copy(
            src_ref=src,
            dst_ref=dst,
            send_sem=rs_send.at[step],
            recv_sem=rs_recv.at[step],
            device_id={"mp": peer},
            device_id_type=pl.DeviceIdType.MESH,
        )

    mp_sent = []

    def scatter(step, src, dst, at):
        for o in range(1, n_mp):
            peer = (m + o) % n_mp
            theirs = rows(peer * share, share)
            mp_copy(step, src.at[theirs, at], dst.at[n_mp - o, :, at], peer).start()
        mp_sent.append((step, dst.at[pl.ds(1, n_mp - 1), :, at]))

    def scattered(step, dst, at):
        ref = dst.at[pl.ds(1, n_mp - 1), :, at]
        mp_copy(step, ref, ref, (m + 1) % n_mp).wait_recv()

    def total(src, dst, at):
        value = src[mine, at].astype(F32)
        for o in range(1, n_mp):
            value = value + dst[o, :, at].astype(F32)
        return value

    def spread(step, buf, at):
        ref = buf.at[mine, at]
        for o in range(1, n_mp):
            mp_copy(step, ref, ref, (m + o) % n_mp).start()
        mp_sent.append((step, buf.at[pl.ds(0, (n_mp - 1) * share), at]))

    def spread_done(step, buf, at):
        ref = buf.at[pl.ds(0, (n_mp - 1) * share), at]
        mp_copy(step, ref, ref, (m + 1) % n_mp).wait_recv()

    def normed_rows(at):
        return jnp.concatenate([normed[j, at, :] for j in range(feat // 128)], 1)

    hop(W1, 1)
    hop(W2A, 1)

    chunk = patches.shape[0] // 4
    loads[2].wait()

    @pl.loop(0, 4)
    def _(c):
        at = rows(c * chunk, chunk)
        x = patches[at, :].astype(F32)
        mean = jnp.mean(x, -1, keepdims=True)
        r = lax.rsqrt(jnp.mean(x * x, -1, keepdims=True) - mean * mean + EPSILON)
        x = (x - mean) * r
        for j in range(feat // 128):
            normed[j, at, :] = x[:, j * 128 : (j + 1) * 128]
        scale[at, :] = jnp.broadcast_to(r, (chunk, 128))

    loads[3].wait()
    wkv_f32[...] = wkv_raw[...].astype(F32)
    for which in (0, 1):
        shard = wkv_f32[pl.ds(which, rq, stride=2), :].astype(BF)
        wkvg[rows(core * rq, rq), which * HEAD : (which + 1) * HEAD] = shard

    hop(W1, 2)
    hop(W2B, 1)

    blk_src = [i, (i + (n_seq - 9) * (1 - core) + (n_seq - 1) * core) % n_seq]
    blk_src += [(i + n_seq - 2 * d) % n_seq for d in (1, 2, 3, 4)]
    blk_src += [(i + n_seq - 2 * d + 1 - 2 * core) % n_seq for d in (1, 2, 3, 4)]
    own_ids = sample_ids[0:1, rows(i * tok, tok)]
    q_ids = jnp.transpose(jnp.broadcast_to(own_ids, (tok, tok)))
    row = lax.broadcasted_iota(jnp.int32, (tok, tok), 0)
    lane = lax.broadcasted_iota(jnp.int32, (tok, tok), 1)
    for b in range(N_BLOCKS):
        s = blk_src[b]
        ids = jnp.broadcast_to(sample_ids[0:1, rows(s * tok, tok)], (tok, tok))
        allowed = (ids == q_ids) & (s * tok + lane <= i * tok + row)
        bias[:, b * tok : (b + 1) * tok] = jnp.where(allowed, 0.0, -NEGATIVE)

    hop(W1, 3)
    hop(W2A, 2)
    hop(W1, 4)
    hop(W2B, 2)
    hop(W1, 5)
    hop(W2A, 3)
    hop(W2B, 3)
    loads[4].wait()
    hop(WKV, 1)
    gathered(slots(W1, 8), 0)

    for place, step in enumerate((0, -1, 1, -2, 2, -3, 3, 4)):
        chip = (i // 2 + n_seq // 2 + step) % (n_seq // 2)
        pair = [w1g[2 * place + c].astype(F32) for c in (0, 1)]
        for p in range(4):
            at = pl.ds(pl.multiple_of(p * feat + 2 * fs * chip, 2 * fs), 2 * fs)
            for j in range(full):
                first = j * r1 + p * fs
                piece = jnp.concatenate([v[first : first + fs] for v in pair], 0)
                w1n[at, j * 128 : (j + 1) * 128] = piece.astype(BF)
            first = full * r1 + (p % 2) * fs
            piece = jnp.concatenate([v[first : first + fs] for v in pair], 0)
            w1n[at, full * 128 :] = piece[:, (p // 2) * 64 : (p // 2) * 64 + 64].astype(BF)

    acc = jnp.zeros((tok, hid), F32)
    for p in range(4):
        x = normed_rows(pl.ds(p, tok, stride=4)).astype(BF)
        acc = acc + dot(x, w1n[p * feat : (p + 1) * feat, :])
    hidden_pre[...] = acc
    hidden[...] = (acc * 0.5 * (1.0 + lax.erf(acc * 0.7071067811865476))).astype(BF)

    def merge_group(g):
        gathered(w2g.at[pl.ds(0, len(groups[g]))], 1 + g)
        for s in range(2 * groups[g][0], 2 * groups[g][-1] + 2):
            part[:, s * dblk : (s + 1) * dblk] = dot(hidden[...], w2g[s]).astype(BF)
        scatter(g, part, recv, spans[g])

    merge_group(0)
    hop(W2A, 4)
    hop(W2B, 4)
    hop(WQA, 1)
    merge_group(1)
    hop(WKV, 2)
    merge_group(2)
    hop(W2A, 5)
    hop(W2B, 5)
    merge_group(3)
    hop(WQA, 2)

    def sum_group(g):
        scattered(g, recv, spans[g])
        for s in range(spans[g].start, spans[g].stop, 2 * dblk):
            at = slice(s, s + 2 * dblk)
            merged[mine, at] = total(part, recv, at).astype(BF)
        spread(4 + g, merged, spans[g])

    sum_group(0)
    hop(WKV, 3)
    sum_group(1)
    hop(WQB, 1)
    sum_group(2)
    hop(WKV, 4)
    sum_group(3)
    hop(WQA, 3)
    hop(WKV, 5)
    hop(WQB, 2)
    hop(WQA, 4)
    for g in range(4):
        spread_done(4 + g, merged, spans[g])

    @pl.loop(0, tok // 16)
    def _(c):
        at = rows(c * 16, 16)
        x = merged[at, :].astype(F32)
        r = lax.rsqrt(jnp.mean(x * x, -1, keepdims=True) + EPSILON)
        row_scale[at, :] = jnp.broadcast_to(r, (16, 128))

    hop(WQB, 3)
    gathered(slots(WKV, 8), 5)
    kv = dot(merged[...], wkvg[...]) * row_scale[:, 0:1]
    keys[0:tok, :] = kv[:, :HEAD].astype(BF)
    values[0:tok, :] = kv[:, HEAD:].astype(BF)

    near = core * ((i + 9) % n_seq) + (1 - core) * sib

    def block(buf, b):
        return buf.at[b * tok : (b + 1) * tok]

    def kv_copy(which, src, dst, arrive, target):
        return seq_copy(src, dst, kv_send.at[which], kv_recv.at[which, arrive], target)

    def kv_step(d):
        for which in (0, 1):
            buf = (keys, values)[which]
            ref = block(buf, 1 + d)
            kv_copy(which, ref, ref, d, sib).wait_recv()
            if d == 1:
                kv_copy(which, ref, block(buf, 4), 3, up2).start()
            kv_copy(which, ref, block(buf, 5 + d), 5, sib).start()

    for which in (0, 1):
        own = block((keys, values)[which], 0)
        kv_copy(which, own, block((keys, values)[which], 2), 1, up).start()
        kv_copy(which, own, kv_relay.at[which], 0, down2).start()
    for which in (0, 1):
        own = block((keys, values)[which], 0)
        kv_copy(which, own, block((keys, values)[which], 3), 2, up2).start()
        kv_copy(which, own, block((keys, values)[which], 1), 5, near).start()
    kv_step(1)
    hop(WQB, 4)
    for which in (0, 1):
        ref = kv_relay.at[which]
        kv_copy(which, ref, ref, 0, sib).wait_recv()
        kv_copy(which, ref, block((keys, values)[which], 5), 4, down2).start()
    hop(WQA, 5)
    kv_step(2)
    kv_step(3)
    kv_step(4)
    hop(WQB, 5)
    gathered(wqg.at[pl.ds(0, 8 * rq)], 6)
    per_kv = qw // HEAD
    for h in range(per_kv):
        at = slice(h * HEAD, (h + 1) * HEAD)
        query[h * tok : (h + 1) * tok, :] = (dot(merged[...], wqg[:, at]) * row_scale[...]).astype(BF)
    for which in (0, 1):
        ref = (keys, values)[which].at[0 : 5 * tok]
        kv_copy(which, ref, ref, 5, sib).wait_recv()

    loads[5].wait()
    score_scale = HEAD ** (-0.5)

    for h in range(per_kv):
        at = slice(h * HEAD, (h + 1) * HEAD)
        q = query[h * tok : (h + 1) * tok, :]
        g = attn_grad[:, at]
        s = dot_nt(q, keys[...]) * score_scale + bias[...]
        e = jnp.exp(s - jnp.max(s, -1, keepdims=True))
        soft = e * (1.0 / jnp.sum(e, -1, keepdims=True))
        soft_bf = soft.astype(BF)
        attended = dot(soft_bf, values[...])
        delta = jnp.sum(g.astype(F32) * attended, -1, keepdims=True)
        dprob = dot_nt(g, values[...])
        ds = (soft * (dprob - delta)).astype(BF)
        dquery[:, at] = (dot(ds, keys[...]) * score_scale).astype(BF)
        dk = dot_tn(ds, q) * score_scale
        dv = dot_tn(soft_bf, g)
        dkeys[...] = dk if h == 0 else dkeys[...] + dk
        dvalues[...] = dv if h == 0 else dvalues[...] + dv

    grads = (dkeys, dvalues)
    back = core * sib + (1 - core) * far

    def ret_copy(which, src, dst, arrive, target):
        return seq_copy(src, dst, ret_ssem.at[which], ret_rsem.at[which, arrive], target)

    def ret_wait(which, ref, arrive):
        ret_copy(which, ref, ref, arrive, sib).wait_recv()

    for which in (0, 1):
        ret_send[which] = grads[which][6 * tok :, :].astype(BF)
        ret_copy(which, ret_send.at[which], ret_recv.at[which], 0, sib).start()
    for which in (0, 1):
        blk_send[which] = grads[which][tok : 2 * tok, :].astype(BF)
        ret_copy(which, blk_send.at[which], blk_recv.at[which], 1, back).start()

    def chain_step(which, d):
        value = grads[which][(1 + d) * tok : (2 + d) * tok, :]
        value = value + ret_recv[which, (d - 1) * tok : d * tok, :].astype(F32)
        if d == 1:
            ret_wait(which, chain_recv.at[which, 2], 4)
            value = value + chain_recv[which, 2].astype(F32)
        chain_send[which, d - 1] = value.astype(BF)
        src, dst = chain_send.at[which, d - 1], chain_recv.at[which, d - 1]
        if d == 4:
            ret_copy(which, src, ret_relay.at[which], 6, up2).start()
        else:
            ret_copy(which, src, dst, 1 + d, down if d == 1 else down2).start()

    for which in (0, 1):
        ret_wait(which, ret_recv.at[which], 0)
        chain_step(which, 3)
        chain_step(which, 4)
    for which in (0, 1):
        chain_step(which, 2)
    half = n_seq // 2
    for s in range(half):
        at = slice(s * dblk, (s + 1) * dblk)
        dn_acc[:, at] = dot_nt(dquery[...], wqg[at, :])
    for which in (0, 1):
        chain_step(which, 1)
    for which in (0, 1):
        ret_wait(which, ret_relay.at[which], 6)
        ret_copy(which, ret_relay.at[which], chain_recv.at[which, 3], 5, up2).start()
    for s in range(half, n_seq):
        at = slice(s * dblk, (s + 1) * dblk)
        dn_acc[:, at] = dot_nt(dquery[...], wqg[at, :])
    for which in (0, 1):
        ret_wait(which, blk_recv.at[which], 1)
        value = grads[which][0:tok, :] + blk_recv[which].astype(F32)
        for d in (2, 4, 1):
            ret_wait(which, chain_recv.at[which, d - 1], 1 + d)
            value = value + chain_recv[which, d - 1].astype(F32)
        grads_kv[:, which * HEAD : (which + 1) * HEAD] = value.astype(BF)

    n_x = n_mp // 2
    z, x_id = m // n_x, m % n_x
    z_peer = (m + n_x) % n_mp
    col_b = spans[0]
    col_a = slice(spans[1].start, spans[3].stop)

    def x_peer(o):
        return z * n_x + (x_id + o) % n_x

    def block_rows(zz, xx):
        return rows((zz * n_x + xx) * share, share)

    def rs_copy(src, dst, arrive, peer):
        return pltpu.make_async_remote_copy(
            src_ref=src,
            dst_ref=dst,
            send_sem=rs_send.at[8],
            recv_sem=rs_recv.at[8 + arrive],
            device_id={"mp": peer},
            device_id_type=pl.DeviceIdType.MESH,
        )

    def rs_wait(ref, arrive):
        rs_copy(ref, ref, arrive, z_peer).wait_recv()

    for g in (1, 2, 3, 0):
        for s in range(2 * groups[g][0], 2 * groups[g][-1] + 2):
            at = slice(s * dblk, (s + 1) * dblk)
            part2[:, at] = (dn_acc[:, at] + dot_nt(grads_kv[...], wkvg[at, :])).astype(BF)
        if g > 0:
            for xx in range(n_x):
                rs_copy(
                    part2.at[block_rows(1 - z, xx), spans[g]], recv2.at[xx, :, spans[g]], g, z_peer
                ).start()
        else:
            for o in range(1, n_x):
                for zz in range(2):
                    rs_copy(
                        part2.at[block_rows(zz, (x_id + o) % n_x), col_b],
                        recv2.at[2 * (n_x - o) + zz, :, col_b],
                        0,
                        x_peer(o),
                    ).start()
    def sum_a(xx, at):
        return part2[block_rows(z, xx), at].astype(F32) + recv2[xx, :, at].astype(F32)

    for g in (1, 2, 3):
        rs_wait(recv2.at[pl.ds(0, n_x), :, spans[g]], g)
        for o in range(1, n_x):
            sum2[o, :, spans[g]] = sum_a((x_id + o) % n_x, spans[g]).astype(BF)
            rs_copy(sum2.at[o, :, spans[g]], recv2.at[2 * n_x - o, :, spans[g]], 4, x_peer(o)).start()
    rs_wait(recv2.at[pl.ds(2, 2 * n_x - 2), :, col_b], 0)

    def sum_b(zz):
        value = part2[block_rows(zz, x_id), col_b].astype(F32)
        for o in range(1, n_x):
            value = value + recv2[2 * o + zz, :, col_b].astype(F32)
        return value

    sum2[0, :, col_b] = sum_b(1 - z).astype(BF)
    rs_copy(sum2.at[0, :, col_b], recv2.at[0, :, col_b], 5, z_peer).start()
    dn_a, dn_b = sum_a(x_id, col_a), sum_b(z)
    rs_wait(recv2.at[pl.ds(n_x + 1, n_x - 1), :, col_a], 4)
    for o in range(1, n_x):
        dn_a = dn_a + recv2[n_x + o, :, col_a].astype(F32)
    rs_wait(recv2.at[0, :, col_b], 5)
    dn_b = dn_b + recv2[0, :, col_b].astype(F32)
    x = merged[mine, :].astype(F32)
    r = lax.rsqrt(jnp.mean(x * x, -1, keepdims=True) + EPSILON)
    x = x * r
    dn = jnp.concatenate([dn_b, dn_a], 1)
    dmerged[mine, :] = (r * (dn - x * jnp.mean(dn * x, -1, keepdims=True))).astype(BF)

    def ag_copy(block, at, arrive, peer):
        ref = dmerged.at[block, at]
        return pltpu.make_async_remote_copy(
            src_ref=ref,
            dst_ref=ref,
            send_sem=rs_send.at[9],
            recv_sem=rs_recv.at[20 + arrive],
            device_id={"mp": peer},
            device_id_type=pl.DeviceIdType.MESH,
        )

    ag_copy(mine, col_b, 0, z_peer).start()
    for o in range(1, n_x):
        ag_copy(mine, col_a, n_x - o, x_peer(o)).start()
    ag_copy(mine, col_a, 4, z_peer).start()
    for o in range(1, n_x):
        ag_copy(mine, col_b, 5, x_peer(o)).start()
    theirs = rows(z_peer * share, share)
    ag_copy(theirs, col_b, 0, z_peer).wait_recv()
    for o in range(1, n_x):
        ag_copy(theirs, col_b, 5, x_peer(o)).start()
    for o in (1, 3, 2):
        block_of = rows(x_peer(o) * share, share)
        ag_copy(block_of, col_a, o, z_peer).wait_recv()
        ag_copy(block_of, col_a, 4, z_peer).start()
    acc = jnp.zeros((tok, hid), F32)
    ag_copy(pl.ds(0, (2 * n_x - 2) * share), col_b, 5, z_peer).wait_recv()
    for s in range(2 * groups[0][0], 2 * groups[0][-1] + 2):
        acc = acc + dot_nt(dmerged[:, s * dblk : (s + 1) * dblk], w2g[s])
    ag_copy(pl.ds(0, n_x * share), col_a, 4, z_peer).wait_recv()
    for s in range(2 * groups[1][0], n_seq):
        acc = acc + dot_nt(dmerged[:, s * dblk : (s + 1) * dblk], w2g[s])
    dhidden = (acc * gelu_grad(hidden_pre[...])).astype(BF)
    pieces = [slice(p * feat, (p + 1) * feat) for p in range(4)]
    for p in range(4):
        part3[:, pieces[p]] = dot_nt(dhidden, w1n[pieces[p], :]).astype(BF)
        scatter(16 + p, part3, recv3, pieces[p])
    for p in range(4):
        scattered(16 + p, recv3, pieces[p])
        dx = total(part3, recv3, pieces[p])
        own = pl.ds(m * (4 * share) + p, share, stride=4)
        nx = normed_rows(own)
        first = jnp.mean(dx, -1, keepdims=True)
        second = jnp.mean(dx * nx, -1, keepdims=True)
        dx = scale[own, :][:, 0:1] * (dx - first - nx * second)
        for j in range(feat // 128):
            out_f32[j, pl.ds(p, share, stride=4), :] = dx[:, j * 128 : (j + 1) * 128]
    for j in range(feat // 128):
        out[:, j * 128 : (j + 1) * 128] = out_f32[j].astype(BF)

    for p in range(6):
        seq_copy(slots(p, 15), slots(p, 15), w_send.at[p], w_recv.at[p, 0], sib).wait_send()
    for step, ref in mp_sent:
        mp_copy(step, ref, ref, (m + 1) % n_mp).wait_send()
    both = dmerged.at[pl.ds(0, (n_mp - 1) * share)]
    rs_copy(both, both, 0, z_peer).wait_send()
    ag_copy(pl.ds(0, (n_mp - 1) * share), slice(0, n_seq * dblk), 0, z_peer).wait_send()
    for which in (0, 1):
        kv_copy(which, keys, keys, 0, sib).wait_send()
        ret_copy(which, keys, keys, 0, sib).wait_send()


def local(patches, w_merge1, w_merge2, w_query, w_keyval, attn_grad, sample_ids):
    n_seq, n_mp = lax.axis_size("seq"), lax.axis_size("mp")
    w1 = w_merge1.reshape(-1, w_merge1.shape[2])
    wkv = w_keyval.reshape(-1, HEAD)
    tok = attn_grad.shape[0]
    share = tok // n_mp
    feat = patches.shape[1]
    hid = w1.shape[1]
    width = n_seq * w_query.shape[0]
    qw = w_query.shape[1]
    span = N_BLOCKS * tok
    scratch = [
        pltpu.VMEM(patches.shape, BF),
        pltpu.VMEM(attn_grad.shape, BF),
        pltpu.VMEM(wkv.shape, BF),
        pltpu.VMEM(wkv.shape, F32),
        pltpu.VMEM(w1.shape, BF),
        pltpu.VMEM((n_seq, w1.size // 128, 128), BF),
        pltpu.VMEM((4 * feat, hid), BF),
        pltpu.VMEM((n_seq, *w_merge2.shape), BF),
        pltpu.VMEM((width, qw), BF),
        pltpu.VMEM((width, 2 * HEAD), BF),
        pltpu.VMEM((feat // 128, 4 * tok, 128), F32),
        pltpu.VMEM((4 * tok, 128), F32),
        pltpu.VMEM((tok, hid), F32),
        pltpu.VMEM((tok, hid), BF),
        pltpu.VMEM((tok, width), BF),
        pltpu.VMEM((n_mp, share, width), BF),
        pltpu.VMEM((tok, width), BF),
        pltpu.VMEM((tok, 128), F32),
        pltpu.VMEM((qw // HEAD * tok, HEAD), BF),
        pltpu.VMEM((span, HEAD), BF),
        pltpu.VMEM((span, HEAD), BF),
        pltpu.VMEM((tok, span), F32),
        pltpu.VMEM((span, HEAD), F32),
        pltpu.VMEM((span, HEAD), F32),
        pltpu.VMEM((2, 4 * tok, HEAD), BF),
        pltpu.VMEM((2, 4 * tok, HEAD), BF),
        pltpu.VMEM((2, 4, tok, HEAD), BF),
        pltpu.VMEM((2, 4, tok, HEAD), BF),
        pltpu.VMEM((2, tok, HEAD), BF),
        pltpu.VMEM((2, tok, HEAD), BF),
        pltpu.VMEM((2, tok, HEAD), BF),
        pltpu.VMEM((2, tok, HEAD), BF),
        pltpu.VMEM((tok, qw), BF),
        pltpu.VMEM((tok, 2 * HEAD), BF),
        pltpu.VMEM((tok, width), F32),
        pltpu.VMEM((tok, width), BF),
        pltpu.VMEM((n_mp, share, width), BF),
        pltpu.VMEM((n_mp // 2, share, width), BF),
        pltpu.VMEM((tok, width), BF),
        pltpu.VMEM((tok, 4 * feat), BF),
        pltpu.VMEM((n_mp, share, 4 * feat), BF),
        pltpu.VMEM((feat // 128, 4 * share, 128), F32),
        pltpu.SemaphoreType.DMA((6,)),
        pltpu.SemaphoreType.DMA((6,)),
        pltpu.SemaphoreType.DMA((6, 4)),
        pltpu.SemaphoreType.DMA((7,)),
        pltpu.SemaphoreType.DMA((20,)),
        pltpu.SemaphoreType.DMA((26,)),
        pltpu.SemaphoreType.DMA((2,)),
        pltpu.SemaphoreType.DMA((2, 6)),
        pltpu.SemaphoreType.DMA((2,)),
        pltpu.SemaphoreType.DMA((2, 7)),
    ]
    vmem = pl.BlockSpec(memory_space=pltpu.VMEM)
    return pl.pallas_call(
        functools.partial(kernel, n_seq, n_mp),
        out_shape=jax.ShapeDtypeStruct((4 * share, feat), BF),
        in_specs=[pl.BlockSpec(memory_space=pl.ANY)] * 6 + [vmem],
        out_specs=vmem,
        scratch_shapes=scratch,
        compiler_params=pltpu.CompilerParams(
            collective_id=0, has_side_effects=True, vmem_limit_bytes=56 * 1024 * 1024
        ),
        name="merger",
    )(patches, w1, w_merge2, w_query, wkv, attn_grad, sample_ids)


def solution(mesh):
    in_specs = (
        P(("group", "seq"), None),
        P(None, "seq", "mp"),
        P("mp", "seq"),
        P("seq", "mp"),
        P("seq", None, "mp"),
        P(("group", "seq"), "mp"),
        P("group", None),
    )
    out_specs = P(("group", "seq", "mp"), None)
    return jax.shard_map(local, mesh=mesh, in_specs=in_specs, out_specs=out_specs, check_vma=False)
```

```python
import functools

import jax
import jax.numpy as jnp
from jax import lax
from jax.experimental import pallas as pl
from jax.experimental.pallas import tpu as pltpu
from jax.sharding import PartitionSpec as P

HEAD = 128
EPSILON = 1e-06
NEGATIVE = 1e30
BF = jnp.bfloat16
F32 = jnp.float32
N_BLOCKS = 10


def gelu_grad(inputs):
    normal_cdf = 0.5 * (1.0 + lax.erf(inputs * 0.7071067811865476))
    normal_pdf = jnp.exp(-0.5 * inputs * inputs) * 0.3989422804014327
    return normal_cdf + inputs * normal_pdf


def dot(a, b):
    return jnp.dot(a, b, preferred_element_type=F32)


def dot_nt(a, b):
    return lax.dot_general(a, b, (((1,), (1,)), ((), ())), preferred_element_type=F32)


def dot_tn(a, b):
    return lax.dot_general(a, b, (((0,), (0,)), ((), ())), preferred_element_type=F32)


def rows(start, count):
    return pl.ds(pl.multiple_of(start, count), count)


def kernel(
    n_seq,
    n_mp,
    patches_hbm,
    w1_hbm,
    w2_hbm,
    wq_hbm,
    wkv_hbm,
    attn_grad_hbm,
    sample_ids,
    out,
    patches,
    attn_grad,
    wkv_raw,
    wkv_f32,
    w1_raw,
    w1g,
    w1n,
    w2g,
    wqg,
    wkvg,
    normed,
    scale,
    hidden_pre,
    hidden,
    part,
    recv,
    merged,
    row_scale,
    query,
    keys,
    values,
    bias,
    dkeys,
    dvalues,
    ret_send,
    ret_recv,
    chain_send,
    chain_recv,
    blk_send,
    blk_recv,
    kv_relay,
    ret_relay,
    dquery,
    grads_kv,
    dn_acc,
    part2,
    recv2,
    sum2,
    dmerged,
    part3,
    recv3,
    out_f32,
    in_sem,
    w_send,
    w_recv,
    w_sib,
    rs_send,
    rs_recv,
    kv_send,
    kv_recv,
    ret_ssem,
    ret_rsem,
):
    i = lax.axis_index("seq")
    m = lax.axis_index("mp")
    core = i % 2
    sib = i + 1 - 2 * core
    up = (i + 2) % n_seq
    down = (i + n_seq - 2) % n_seq
    up2 = (i + 4) % n_seq
    down2 = (i + n_seq - 4) % n_seq
    far = (i + 9 * core + (n_seq - 9) * (1 - core)) % n_seq
    tok, qw = attn_grad.shape
    share = tok // n_mp
    feat = patches.shape[1]
    fs = feat // n_seq
    hid = hidden.shape[1]
    dblk = w2g.shape[2]
    mine = rows(m * share, share)

    def seq_copy(src, dst, ssem, rsem, target):
        return pltpu.make_async_remote_copy(
            src_ref=src,
            dst_ref=dst,
            send_sem=ssem,
            recv_sem=rsem,
            device_id={"seq": target},
            device_id_type=pl.DeviceIdType.MESH,
        )

    barrier = pltpu.get_barrier_semaphore()
    for target in (up, down, up2, down2, sib, far):
        pl.semaphore_signal(
            barrier, inc=1, device_id={"seq": target}, device_id_type=pl.DeviceIdType.MESH
        )
    for o in range(1, n_mp):
        pl.semaphore_signal(
            barrier,
            inc=1,
            device_id={"mp": (m + o) % n_mp},
            device_id_type=pl.DeviceIdType.MESH,
        )

    groups = [(range(0, 3)), (range(3, 5)), (range(5, 7)), (range(7, 8))]
    spans = [slice(2 * g[0] * dblk, (2 * g[-1] + 2) * dblk) for g in groups]

    half2 = w2g.shape[1] // 2
    rq = wqg.shape[0] // n_seq
    W1, W2A, W2B, WKV, WQA, WQB = range(6)

    def slot(p, s):
        if p == W1:
            return w1g.at[s]
        if p in (W2A, W2B):
            return w2g.at[s, pl.ds((p - W2A) * half2, half2)]
        if p == WKV:
            return wkvg.at[rows(s * rq, rq)]
        return wqg.at[pl.ds(pl.multiple_of(s * rq + (p - WQA) * (rq // 2), rq // 2), rq // 2)]

    own_q = wqg.at[rows(core * rq, rq)]
    loads = [
        pltpu.make_async_copy(w1_hbm, w1_raw, in_sem.at[0]),
        pltpu.make_async_copy(w2_hbm, w2g.at[core], in_sem.at[1]),
        pltpu.make_async_copy(patches_hbm, patches, in_sem.at[2]),
        pltpu.make_async_copy(wkv_hbm, wkv_raw, in_sem.at[3]),
        pltpu.make_async_copy(wq_hbm, own_q, in_sem.at[4]),
        pltpu.make_async_copy(attn_grad_hbm, attn_grad, in_sem.at[5]),
    ]
    for load in loads:
        load.start()
    loads[0].wait()
    r1 = w1_raw.shape[0]
    full = hid // 128
    for j in range(full):
        w1g[core, j * r1 : (j + 1) * r1, :] = w1_raw[:, j * 128 : (j + 1) * 128]
    tail = w1_raw[:, full * 128 :].astype(F32)
    w1g[core, full * r1 :, :] = jnp.concatenate([tail[: r1 // 2], tail[r1 // 2 :]], 1).astype(BF)
    loads[1].wait()
    pl.semaphore_wait(barrier, 6 + n_mp - 1)

    def slots(p, count):
        if p == W1:
            return w1g.at[pl.ds(0, count)]
        if p in (W2A, W2B):
            return w2g.at[pl.ds(0, count), pl.ds((p - W2A) * half2, half2)]
        if p == WKV:
            return wkvg.at[pl.ds(0, count * rq)]
        return wqg.at[pl.ds(0, count * (rq // 2))]

    def ring(p, src_place, dst_place, target):
        seq_copy(
            slot(p, 2 * src_place + core),
            slot(p, 2 * dst_place + core),
            w_send.at[p],
            w_recv.at[p, (dst_place - 1) // 2],
            target,
        ).start()

    def sib_sem(p, place):
        if p == W1:
            return w_sib.at[0]
        if p in (W2A, W2B):
            return w_sib.at[1 + [k for k in range(4) if place in groups[k]][0]]
        return w_sib.at[5 if p == WKV else 6]

    def to_sib(p, place):
        ref = slot(p, 2 * place + core)
        seq_copy(ref, ref, w_send.at[p], sib_sem(p, place), sib).start()

    def arrived(p, step):
        ref = slots(p, 1 if step == 3 else 2)
        seq_copy(ref, ref, w_send.at[p], w_recv.at[p, step], sib).wait_recv()

    turn = core * down + (1 - core) * up

    def hop(p, h):
        if h == 1:
            ring(p, 0, 1, up)
            ring(p, 0, 2, down)
            to_sib(p, 0)
            return
        arrived(p, h - 2)
        if h <= 3:
            ring(p, 2 * h - 3, 2 * h - 1, up)
            ring(p, 2 * h - 2, 2 * h, down)
        elif h == 4:
            ring(p, 5 + core, 7, turn)
        if h <= 4:
            to_sib(p, 2 * h - 3)
            to_sib(p, 2 * h - 2)
        else:
            to_sib(p, 7)

    def gathered(ref, sem):
        seq_copy(ref, ref, w_send.at[0], w_sib.at[sem], sib).wait_recv()

    def mp_copy(step, src, dst, peer):
        return pltpu.make_async_remote_copy(
            src_ref=src,
            dst_ref=dst,
            send_sem=rs_send.at[step],
            recv_sem=rs_recv.at[step],
            device_id={"mp": peer},
            device_id_type=pl.DeviceIdType.MESH,
        )

    mp_sent = []

    def scatter(step, src, dst, at):
        for o in range(1, n_mp):
            peer = (m + o) % n_mp
            theirs = rows(peer * share, share)
            mp_copy(step, src.at[theirs, at], dst.at[n_mp - o, :, at], peer).start()
        mp_sent.append((step, dst.at[pl.ds(1, n_mp - 1), :, at]))

    def scattered(step, dst, at):
        ref = dst.at[pl.ds(1, n_mp - 1), :, at]
        mp_copy(step, ref, ref, (m + 1) % n_mp).wait_recv()

    def total(src, dst, at):
        value = src[mine, at].astype(F32)
        for o in range(1, n_mp):
            value = value + dst[o, :, at].astype(F32)
        return value

    def spread(step, buf, at):
        ref = buf.at[mine, at]
        for o in range(1, n_mp):
            mp_copy(step, ref, ref, (m + o) % n_mp).start()
        mp_sent.append((step, buf.at[pl.ds(0, (n_mp - 1) * share), at]))

    def spread_done(step, buf, at):
        ref = buf.at[pl.ds(0, (n_mp - 1) * share), at]
        mp_copy(step, ref, ref, (m + 1) % n_mp).wait_recv()

    def normed_rows(at):
        return jnp.concatenate([normed[j, at, :] for j in range(feat // 128)], 1)

    hop(W1, 1)
    hop(W2A, 1)

    chunk = patches.shape[0] // 4
    loads[2].wait()

    @pl.loop(0, 4)
    def _(c):
        at = rows(c * chunk, chunk)
        x = patches[at, :].astype(F32)
        mean = jnp.mean(x, -1, keepdims=True)
        r = lax.rsqrt(jnp.mean(x * x, -1, keepdims=True) - mean * mean + EPSILON)
        x = (x - mean) * r
        for j in range(feat // 128):
            normed[j, at, :] = x[:, j * 128 : (j + 1) * 128]
        scale[at, :] = jnp.broadcast_to(r, (chunk, 128))

    loads[3].wait()
    wkv_f32[...] = wkv_raw[...].astype(F32)
    for which in (0, 1):
        shard = wkv_f32[pl.ds(which, rq, stride=2), :].astype(BF)
        wkvg[rows(core * rq, rq), which * HEAD : (which + 1) * HEAD] = shard

    hop(W1, 2)
    hop(W2B, 1)

    blk_src = [i, (i + (n_seq - 9) * (1 - core) + (n_seq - 1) * core) % n_seq]
    blk_src += [(i + n_seq - 2 * d) % n_seq for d in (1, 2, 3, 4)]
    blk_src += [(i + n_seq - 2 * d + 1 - 2 * core) % n_seq for d in (1, 2, 3, 4)]
    own_ids = sample_ids[0:1, rows(i * tok, tok)]
    q_ids = jnp.transpose(jnp.broadcast_to(own_ids, (tok, tok)))
    row = lax.broadcasted_iota(jnp.int32, (tok, tok), 0)
    lane = lax.broadcasted_iota(jnp.int32, (tok, tok), 1)
    for b in range(N_BLOCKS):
        s = blk_src[b]
        ids = jnp.broadcast_to(sample_ids[0:1, rows(s * tok, tok)], (tok, tok))
        allowed = (ids == q_ids) & (s * tok + lane <= i * tok + row)
        bias[:, b * tok : (b + 1) * tok] = jnp.where(allowed, 0.0, -NEGATIVE)

    hop(W1, 3)
    hop(W2A, 2)
    hop(W1, 4)
    hop(W2B, 2)
    hop(W1, 5)
    hop(W2A, 3)
    hop(W2B, 3)
    loads[4].wait()
    hop(WKV, 1)
    gathered(slots(W1, 8), 0)

    for place, step in enumerate((0, -1, 1, -2, 2, -3, 3, 4)):
        chip = (i // 2 + n_seq // 2 + step) % (n_seq // 2)
        pair = [w1g[2 * place + c].astype(F32) for c in (0, 1)]
        for p in range(4):
            at = pl.ds(pl.multiple_of(p * feat + 2 * fs * chip, 2 * fs), 2 * fs)
            for j in range(full):
                first = j * r1 + p * fs
                piece = jnp.concatenate([v[first : first + fs] for v in pair], 0)
                w1n[at, j * 128 : (j + 1) * 128] = piece.astype(BF)
            first = full * r1 + (p % 2) * fs
            piece = jnp.concatenate([v[first : first + fs] for v in pair], 0)
            w1n[at, full * 128 :] = piece[:, (p // 2) * 64 : (p // 2) * 64 + 64].astype(BF)

    acc = jnp.zeros((tok, hid), F32)
    for p in range(4):
        x = normed_rows(pl.ds(p, tok, stride=4)).astype(BF)
        acc = acc + dot(x, w1n[p * feat : (p + 1) * feat, :])
    hidden_pre[...] = acc
    hidden[...] = (acc * 0.5 * (1.0 + lax.erf(acc * 0.7071067811865476))).astype(BF)

    def merge_group(g):
        gathered(w2g.at[pl.ds(0, len(groups[g]))], 1 + g)
        for s in range(2 * groups[g][0], 2 * groups[g][-1] + 2):
            part[:, s * dblk : (s + 1) * dblk] = dot(hidden[...], w2g[s]).astype(BF)
        scatter(g, part, recv, spans[g])

    merge_group(0)
    hop(W2A, 4)
    hop(W2B, 4)
    hop(WQA, 1)
    merge_group(1)
    hop(WKV, 2)
    merge_group(2)
    hop(W2A, 5)
    hop(W2B, 5)
    merge_group(3)
    hop(WQA, 2)

    def sum_group(g):
        scattered(g, recv, spans[g])
        for s in range(spans[g].start, spans[g].stop, 2 * dblk):
            at = slice(s, s + 2 * dblk)
            merged[mine, at] = total(part, recv, at).astype(BF)
        spread(4 + g, merged, spans[g])

    sum_group(0)
    hop(WKV, 3)
    sum_group(1)
    hop(WQB, 1)
    sum_group(2)
    hop(WKV, 4)
    sum_group(3)
    hop(WQA, 3)
    hop(WKV, 5)
    hop(WQB, 2)
    hop(WQA, 4)
    for g in range(4):
        spread_done(4 + g, merged, spans[g])

    @pl.loop(0, tok // 16)
    def _(c):
        at = rows(c * 16, 16)
        x = merged[at, :].astype(F32)
        r = lax.rsqrt(jnp.mean(x * x, -1, keepdims=True) + EPSILON)
        row_scale[at, :] = jnp.broadcast_to(r, (16, 128))

    gathered(slots(WKV, 8), 5)
    kv = dot(merged[...], wkvg[...]) * row_scale[:, 0:1]
    keys[0:tok, :] = kv[:, :HEAD].astype(BF)
    values[0:tok, :] = kv[:, HEAD:].astype(BF)

    near = core * ((i + 9) % n_seq) + (1 - core) * sib

    def block(buf, b):
        return buf.at[b * tok : (b + 1) * tok]

    def kv_copy(which, src, dst, arrive, target):
        return seq_copy(src, dst, kv_send.at[which], kv_recv.at[which, arrive], target)

    def kv_step(d):
        for which in (0, 1):
            buf = (keys, values)[which]
            ref = block(buf, 1 + d)
            kv_copy(which, ref, ref, d, sib).wait_recv()
            if d == 1:
                kv_copy(which, ref, block(buf, 4), 3, up2).start()
            kv_copy(which, ref, block(buf, 5 + d), 5, sib).start()

    for which in (0, 1):
        own = block((keys, values)[which], 0)
        kv_copy(which, own, block((keys, values)[which], 2), 1, up).start()
        kv_copy(which, own, kv_relay.at[which], 0, down2).start()
    hop(WQB, 3)
    for which in (0, 1):
        own = block((keys, values)[which], 0)
        kv_copy(which, own, block((keys, values)[which], 3), 2, up2).start()
        kv_copy(which, own, block((keys, values)[which], 1), 5, near).start()
    kv_step(1)
    for which in (0, 1):
        ref = kv_relay.at[which]
        kv_copy(which, ref, ref, 0, sib).wait_recv()
        kv_copy(which, ref, block((keys, values)[which], 5), 4, down2).start()
    hop(WQB, 4)
    hop(WQA, 5)
    kv_step(2)
    kv_step(3)
    kv_step(4)
    hop(WQB, 5)
    gathered(wqg.at[pl.ds(0, 8 * rq)], 6)
    per_kv = qw // HEAD
    for h in range(per_kv):
        at = slice(h * HEAD, (h + 1) * HEAD)
        query[h * tok : (h + 1) * tok, :] = (dot(merged[...], wqg[:, at]) * row_scale[...]).astype(BF)
    for which in (0, 1):
        ref = (keys, values)[which].at[0 : 5 * tok]
        kv_copy(which, ref, ref, 5, sib).wait_recv()

    loads[5].wait()
    score_scale = HEAD ** (-0.5)

    for h in range(per_kv):
        at = slice(h * HEAD, (h + 1) * HEAD)
        q = query[h * tok : (h + 1) * tok, :]
        g = attn_grad[:, at]
        s = dot_nt(q, keys[...]) * score_scale + bias[...]
        e = jnp.exp(s - jnp.max(s, -1, keepdims=True))
        soft = e * (1.0 / jnp.sum(e, -1, keepdims=True))
        soft_bf = soft.astype(BF)
        attended = dot(soft_bf, values[...])
        delta = jnp.sum(g.astype(F32) * attended, -1, keepdims=True)
        dprob = dot_nt(g, values[...])
        ds = (soft * (dprob - delta)).astype(BF)
        dquery[:, at] = (dot(ds, keys[...]) * score_scale).astype(BF)
        dk = dot_tn(ds, q) * score_scale
        dv = dot_tn(soft_bf, g)
        dkeys[...] = dk if h == 0 else dkeys[...] + dk
        dvalues[...] = dv if h == 0 else dvalues[...] + dv

    grads = (dkeys, dvalues)
    back = core * sib + (1 - core) * far

    def ret_copy(which, src, dst, arrive, target):
        return seq_copy(src, dst, ret_ssem.at[which], ret_rsem.at[which, arrive], target)

    def ret_wait(which, ref, arrive):
        ret_copy(which, ref, ref, arrive, sib).wait_recv()

    for which in (0, 1):
        ret_send[which] = grads[which][6 * tok :, :].astype(BF)
        ret_copy(which, ret_send.at[which], ret_recv.at[which], 0, sib).start()
    for which in (0, 1):
        blk_send[which] = grads[which][tok : 2 * tok, :].astype(BF)
        ret_copy(which, blk_send.at[which], blk_recv.at[which], 1, back).start()

    def chain_step(which, d):
        value = grads[which][(1 + d) * tok : (2 + d) * tok, :]
        value = value + ret_recv[which, (d - 1) * tok : d * tok, :].astype(F32)
        if d == 1:
            ret_wait(which, chain_recv.at[which, 2], 4)
            value = value + chain_recv[which, 2].astype(F32)
        chain_send[which, d - 1] = value.astype(BF)
        src, dst = chain_send.at[which, d - 1], chain_recv.at[which, d - 1]
        if d == 4:
            ret_copy(which, src, ret_relay.at[which], 6, up2).start()
        else:
            ret_copy(which, src, dst, 1 + d, down if d == 1 else down2).start()

    for which in (0, 1):
        ret_wait(which, ret_recv.at[which], 0)
        chain_step(which, 3)
        chain_step(which, 4)
    for which in (0, 1):
        chain_step(which, 2)
    half = n_seq // 2
    for s in range(half):
        at = slice(s * dblk, (s + 1) * dblk)
        dn_acc[:, at] = dot_nt(dquery[...], wqg[at, :])
    for which in (0, 1):
        chain_step(which, 1)
    for which in (0, 1):
        ret_wait(which, ret_relay.at[which], 6)
        ret_copy(which, ret_relay.at[which], chain_recv.at[which, 3], 5, up2).start()
    for s in range(half, n_seq):
        at = slice(s * dblk, (s + 1) * dblk)
        dn_acc[:, at] = dot_nt(dquery[...], wqg[at, :])
    for which in (0, 1):
        ret_wait(which, blk_recv.at[which], 1)
        value = grads[which][0:tok, :] + blk_recv[which].astype(F32)
        for d in (2, 4, 1):
            ret_wait(which, chain_recv.at[which, d - 1], 1 + d)
            value = value + chain_recv[which, d - 1].astype(F32)
        grads_kv[:, which * HEAD : (which + 1) * HEAD] = value.astype(BF)

    n_x = n_mp // 2
    z, x_id = m // n_x, m % n_x
    z_peer = (m + n_x) % n_mp
    col_b = spans[0]
    col_a = slice(spans[1].start, spans[3].stop)

    def x_peer(o):
        return z * n_x + (x_id + o) % n_x

    def block_rows(zz, xx):
        return rows((zz * n_x + xx) * share, share)

    def rs_copy(src, dst, arrive, peer):
        return pltpu.make_async_remote_copy(
            src_ref=src,
            dst_ref=dst,
            send_sem=rs_send.at[8],
            recv_sem=rs_recv.at[8 + arrive],
            device_id={"mp": peer},
            device_id_type=pl.DeviceIdType.MESH,
        )

    def rs_wait(ref, arrive):
        rs_copy(ref, ref, arrive, z_peer).wait_recv()

    for g in (1, 2, 3, 0):
        for s in range(2 * groups[g][0], 2 * groups[g][-1] + 2):
            at = slice(s * dblk, (s + 1) * dblk)
            part2[:, at] = (dn_acc[:, at] + dot_nt(grads_kv[...], wkvg[at, :])).astype(BF)
        if g > 0:
            for xx in range(n_x):
                rs_copy(
                    part2.at[block_rows(1 - z, xx), spans[g]], recv2.at[xx, :, spans[g]], g, z_peer
                ).start()
        else:
            for o in range(1, n_x):
                for zz in range(2):
                    rs_copy(
                        part2.at[block_rows(zz, (x_id + o) % n_x), col_b],
                        recv2.at[2 * (n_x - o) + zz, :, col_b],
                        0,
                        x_peer(o),
                    ).start()
    def sum_a(xx, at):
        return part2[block_rows(z, xx), at].astype(F32) + recv2[xx, :, at].astype(F32)

    for g in (1, 2, 3):
        rs_wait(recv2.at[pl.ds(0, n_x), :, spans[g]], g)
        for o in range(1, n_x):
            sum2[o, :, spans[g]] = sum_a((x_id + o) % n_x, spans[g]).astype(BF)
            rs_copy(sum2.at[o, :, spans[g]], recv2.at[2 * n_x - o, :, spans[g]], 4, x_peer(o)).start()
    rs_wait(recv2.at[pl.ds(2, 2 * n_x - 2), :, col_b], 0)

    def sum_b(zz):
        value = part2[block_rows(zz, x_id), col_b].astype(F32)
        for o in range(1, n_x):
            value = value + recv2[2 * o + zz, :, col_b].astype(F32)
        return value

    sum2[0, :, col_b] = sum_b(1 - z).astype(BF)
    rs_copy(sum2.at[0, :, col_b], recv2.at[0, :, col_b], 5, z_peer).start()
    dn_a, dn_b = sum_a(x_id, col_a), sum_b(z)
    rs_wait(recv2.at[pl.ds(n_x + 1, n_x - 1), :, col_a], 4)
    for o in range(1, n_x):
        dn_a = dn_a + recv2[n_x + o, :, col_a].astype(F32)
    rs_wait(recv2.at[0, :, col_b], 5)
    dn_b = dn_b + recv2[0, :, col_b].astype(F32)
    x = merged[mine, :].astype(F32)
    r = lax.rsqrt(jnp.mean(x * x, -1, keepdims=True) + EPSILON)
    x = x * r
    dn = jnp.concatenate([dn_b, dn_a], 1)
    dmerged[mine, :] = (r * (dn - x * jnp.mean(dn * x, -1, keepdims=True))).astype(BF)

    def ag_copy(block, at, arrive, peer):
        ref = dmerged.at[block, at]
        return pltpu.make_async_remote_copy(
            src_ref=ref,
            dst_ref=ref,
            send_sem=rs_send.at[9],
            recv_sem=rs_recv.at[20 + arrive],
            device_id={"mp": peer},
            device_id_type=pl.DeviceIdType.MESH,
        )

    ag_copy(mine, col_b, 0, z_peer).start()
    for o in range(1, n_x):
        ag_copy(mine, col_a, n_x - o, x_peer(o)).start()
    ag_copy(mine, col_a, 4, z_peer).start()
    for o in range(1, n_x):
        ag_copy(mine, col_b, 5, x_peer(o)).start()
    theirs = rows(z_peer * share, share)
    ag_copy(theirs, col_b, 0, z_peer).wait_recv()
    for o in range(1, n_x):
        ag_copy(theirs, col_b, 5, x_peer(o)).start()
    for o in (1, 3, 2):
        block_of = rows(x_peer(o) * share, share)
        ag_copy(block_of, col_a, o, z_peer).wait_recv()
        ag_copy(block_of, col_a, 4, z_peer).start()
    acc = jnp.zeros((tok, hid), F32)
    ag_copy(pl.ds(0, (2 * n_x - 2) * share), col_b, 5, z_peer).wait_recv()
    for s in range(2 * groups[0][0], 2 * groups[0][-1] + 2):
        acc = acc + dot_nt(dmerged[:, s * dblk : (s + 1) * dblk], w2g[s])
    ag_copy(pl.ds(0, n_x * share), col_a, 4, z_peer).wait_recv()
    for s in range(2 * groups[1][0], n_seq):
        acc = acc + dot_nt(dmerged[:, s * dblk : (s + 1) * dblk], w2g[s])
    dhidden = (acc * gelu_grad(hidden_pre[...])).astype(BF)
    pieces = [slice(p * feat, (p + 1) * feat) for p in range(4)]
    for p in range(4):
        part3[:, pieces[p]] = dot_nt(dhidden, w1n[pieces[p], :]).astype(BF)
        scatter(16 + p, part3, recv3, pieces[p])
    for p in range(4):
        scattered(16 + p, recv3, pieces[p])
        dx = total(part3, recv3, pieces[p])
        own = pl.ds(m * (4 * share) + p, share, stride=4)
        nx = normed_rows(own)
        first = jnp.mean(dx, -1, keepdims=True)
        second = jnp.mean(dx * nx, -1, keepdims=True)
        dx = scale[own, :][:, 0:1] * (dx - first - nx * second)
        for j in range(feat // 128):
            out_f32[j, pl.ds(p, share, stride=4), :] = dx[:, j * 128 : (j + 1) * 128]
    for j in range(feat // 128):
        out[:, j * 128 : (j + 1) * 128] = out_f32[j].astype(BF)

    for p in range(6):
        seq_copy(slots(p, 15), slots(p, 15), w_send.at[p], w_recv.at[p, 0], sib).wait_send()
    for step, ref in mp_sent:
        mp_copy(step, ref, ref, (m + 1) % n_mp).wait_send()
    both = dmerged.at[pl.ds(0, (n_mp - 1) * share)]
    rs_copy(both, both, 0, z_peer).wait_send()
    ag_copy(pl.ds(0, (n_mp - 1) * share), slice(0, n_seq * dblk), 0, z_peer).wait_send()
    for which in (0, 1):
        kv_copy(which, keys, keys, 0, sib).wait_send()
        ret_copy(which, keys, keys, 0, sib).wait_send()


def local(patches, w_merge1, w_merge2, w_query, w_keyval, attn_grad, sample_ids):
    n_seq, n_mp = lax.axis_size("seq"), lax.axis_size("mp")
    w1 = w_merge1.reshape(-1, w_merge1.shape[2])
    wkv = w_keyval.reshape(-1, HEAD)
    tok = attn_grad.shape[0]
    share = tok // n_mp
    feat = patches.shape[1]
    hid = w1.shape[1]
    width = n_seq * w_query.shape[0]
    qw = w_query.shape[1]
    span = N_BLOCKS * tok
    scratch = [
        pltpu.VMEM(patches.shape, BF),
        pltpu.VMEM(attn_grad.shape, BF),
        pltpu.VMEM(wkv.shape, BF),
        pltpu.VMEM(wkv.shape, F32),
        pltpu.VMEM(w1.shape, BF),
        pltpu.VMEM((n_seq, w1.size // 128, 128), BF),
        pltpu.VMEM((4 * feat, hid), BF),
        pltpu.VMEM((n_seq, *w_merge2.shape), BF),
        pltpu.VMEM((width, qw), BF),
        pltpu.VMEM((width, 2 * HEAD), BF),
        pltpu.VMEM((feat // 128, 4 * tok, 128), F32),
        pltpu.VMEM((4 * tok, 128), F32),
        pltpu.VMEM((tok, hid), F32),
        pltpu.VMEM((tok, hid), BF),
        pltpu.VMEM((tok, width), BF),
        pltpu.VMEM((n_mp, share, width), BF),
        pltpu.VMEM((tok, width), BF),
        pltpu.VMEM((tok, 128), F32),
        pltpu.VMEM((qw // HEAD * tok, HEAD), BF),
        pltpu.VMEM((span, HEAD), BF),
        pltpu.VMEM((span, HEAD), BF),
        pltpu.VMEM((tok, span), F32),
        pltpu.VMEM((span, HEAD), F32),
        pltpu.VMEM((span, HEAD), F32),
        pltpu.VMEM((2, 4 * tok, HEAD), BF),
        pltpu.VMEM((2, 4 * tok, HEAD), BF),
        pltpu.VMEM((2, 4, tok, HEAD), BF),
        pltpu.VMEM((2, 4, tok, HEAD), BF),
        pltpu.VMEM((2, tok, HEAD), BF),
        pltpu.VMEM((2, tok, HEAD), BF),
        pltpu.VMEM((2, tok, HEAD), BF),
        pltpu.VMEM((2, tok, HEAD), BF),
        pltpu.VMEM((tok, qw), BF),
        pltpu.VMEM((tok, 2 * HEAD), BF),
        pltpu.VMEM((tok, width), F32),
        pltpu.VMEM((tok, width), BF),
        pltpu.VMEM((n_mp, share, width), BF),
        pltpu.VMEM((n_mp // 2, share, width), BF),
        pltpu.VMEM((tok, width), BF),
        pltpu.VMEM((tok, 4 * feat), BF),
        pltpu.VMEM((n_mp, share, 4 * feat), BF),
        pltpu.VMEM((feat // 128, 4 * share, 128), F32),
        pltpu.SemaphoreType.DMA((6,)),
        pltpu.SemaphoreType.DMA((6,)),
        pltpu.SemaphoreType.DMA((6, 4)),
        pltpu.SemaphoreType.DMA((7,)),
        pltpu.SemaphoreType.DMA((20,)),
        pltpu.SemaphoreType.DMA((26,)),
        pltpu.SemaphoreType.DMA((2,)),
        pltpu.SemaphoreType.DMA((2, 6)),
        pltpu.SemaphoreType.DMA((2,)),
        pltpu.SemaphoreType.DMA((2, 7)),
    ]
    vmem = pl.BlockSpec(memory_space=pltpu.VMEM)
    return pl.pallas_call(
        functools.partial(kernel, n_seq, n_mp),
        out_shape=jax.ShapeDtypeStruct((4 * share, feat), BF),
        in_specs=[pl.BlockSpec(memory_space=pl.ANY)] * 6 + [vmem],
        out_specs=vmem,
        scratch_shapes=scratch,
        compiler_params=pltpu.CompilerParams(
            collective_id=0, has_side_effects=True, vmem_limit_bytes=56 * 1024 * 1024
        ),
        name="merger",
    )(patches, w1, w_merge2, w_query, wkv, attn_grad, sample_ids)


def solution(mesh):
    in_specs = (
        P(("group", "seq"), None),
        P(None, "seq", "mp"),
        P("mp", "seq"),
        P("seq", "mp"),
        P("seq", None, "mp"),
        P(("group", "seq"), "mp"),
        P("group", None),
    )
    out_specs = P(("group", "seq", "mp"), None)
    return jax.shard_map(local, mesh=mesh, in_specs=in_specs, out_specs=out_specs, check_vma=False)
```
